128 devices in a mesh: dp: 32 (over y, z, x_hi), mp: 4 (over x_lo, core).
Axes of the slice: x: 4 (x_hi: 2, x_lo: 2; x = x_hi * 2 + x_lo), y: 4, z: 4, core: 2. Of those that a mesh axis runs over, the one named last changes fastest.
Arguments:
- slow_weights: float32 [1, 3584, 1024], P(None, None, 'mp'), may hold values from -6 to 6
- fast_weights: bfloat16 [32, 1, 3584, 1024], P('dp', None, None, 'mp'), may hold values from -64 to 64
- momentum: float32 [1, 3584, 1024], P(None, None, 'mp'), may hold values from -1.2 to 1.2
Outputs:
- slow_next: float32 [1, 3584, 1024], P(None, None, 'mp')
- momentum_next: float32 [1, 3584, 1024], P(None, None, 'mp')
- fast_next: bfloat16 [32, 1, 3584, 1024], P('dp', None, None, 'mp')
The draws below stay inside these ranges and needn't reach their ends.
All inputs are finite; a program needn't handle non-finite values.
Results may differ from the reference program's by a relative error of at most 0.001.
Values sent between devices are 32-bit elements; how exact they have to be, the bound alone decides.
A program may use at most 64 MiB of HBM per device.

```python
import math
import jax
import jax.numpy as jnp
from jax import lax

D = 3584
LAYERS = 1
KV2 = 1024
REPLICAS = 32


def slow_base(key):
    values = jax.random.normal(jax.random.fold_in(key, 11), (LAYERS, D, KV2), jnp.float32)
    return jnp.clip(values, -6.0, 6.0)


def draw_slow_weights(key, part):
    return slow_base(key)


def draw_fast_weights(key, part):
    slow_values = slow_base(key)
    row_place = jnp.arange(D, dtype=jnp.float32) / D
    col_place = jnp.arange(KV2, dtype=jnp.float32) / KV2
    row_spread = 10.0 ** jax.random.uniform(jax.random.fold_in(key, 12), (D,), jnp.float32)
    col_spread = 10.0 ** jax.random.uniform(jax.random.fold_in(key, 13), (KV2,), jnp.float32)
    common = jax.random.normal(jax.random.fold_in(key, 14), (LAYERS, D, KV2), jnp.float32)
    single = jax.random.normal(jax.random.fold_in(key, 15), (REPLICAS, LAYERS, D, KV2), jnp.float32)
    row_scale = (1.0 + 2.0 * row_place) * row_spread
    col_scale = (1.0 + 2.0 * col_place) * col_spread
    drift = 0.02 * (common[None] + 1.5 * single)
    drift = drift * row_scale[:, None] * col_scale[None, :]
    fast_values = jnp.clip(slow_values[None] - drift, -64.0, 64.0)
    return fast_values.astype(jnp.bfloat16)


def shard_levels(rng, extent, cuts, least, high):
    factor_of = 1.0
    for axis_at, shards_of in cuts:
        heights = jax.random.uniform(jax.random.fold_in(jax.random.fold_in(rng, 6), axis_at), (shards_of,), jnp.float32, least / len(cuts), high / len(cuts))
        factor_of = factor_of * jnp.repeat(jnp.exp(heights), extent[axis_at] // shards_of).reshape((-1,) + (1,) * (len(extent) - 1 - axis_at))
    return factor_of


def gaussian(own_key, dims, deviation, reach, pieces=(), kind=jnp.bfloat16):
    result = jax.random.normal(own_key, dims, jnp.float32) * deviation
    if len(pieces) > 0:
        result = shard_levels(own_key, dims, pieces, -0.22, 0.18) * result
    return jnp.clip(result, min=-reach, max=reach).astype(kind)


def setup_inputs(seed: int = 0) -> dict:
    splits = jax.random.split(jax.random.key(seed), 4)
    return {
        "slow_weights": draw_slow_weights(jax.random.fold_in(splits[3], 71), 0),
        "fast_weights": draw_fast_weights(jax.random.fold_in(splits[3], 71), 0),
        "momentum": gaussian(splits[2], (LAYERS, D, KV2), 0.2, 1.2, ((2, 4),), jnp.float32),
    }


MOMENTUM_RATE = 0.9
OUTER_RATE = 0.7
CLIP_LEVEL = 0.2
EPSILON = 1e-06

def reference(slow_weights, fast_weights, momentum):

    def accumulate(summed, fast_one):
        return (summed + (slow_weights - fast_one.astype(jnp.float32)), None)
    summed, unused = lax.scan(accumulate, jnp.zeros_like(slow_weights), fast_weights)
    pseudo = summed / REPLICAS
    norm_value = jnp.sqrt(jnp.sum(pseudo * pseudo))
    max_norm = CLIP_LEVEL * math.sqrt(LAYERS * D * KV2)
    factor = jnp.minimum(1.0, max_norm / (norm_value + EPSILON))
    gradient = factor * pseudo
    momentum_next = MOMENTUM_RATE * momentum + gradient
    slow_next = slow_weights - OUTER_RATE * (gradient + MOMENTUM_RATE * momentum_next)
    fast_next = jnp.broadcast_to(slow_next.astype(jnp.bfloat16)[None], fast_weights.shape)
    return (slow_next, momentum_next, fast_next)
```

```python
import math

import jax
import jax.numpy as jnp
from jax import lax
from jax.experimental import pallas as pl
from jax.experimental.pallas import tpu as pltpu
from jax.sharding import PartitionSpec as P

MOMENTUM_RATE = 0.9
OUTER_RATE = 0.7
CLIP_LEVEL = 0.2
EPSILON = 1e-06

MESH = pl.DeviceIdType.MESH
UNIT = 256
CHUNKS = (
    ("yzx", 256), ("zyx", 256), ("xyz", 256),
    ("yzx", 256), ("zyx", 256), ("xzy", 256),
    ("yzx", 256), ("zyx", 256), ("xyz", 256),
    ("yzx", 256), ("zyx", 256), ("xzy", 256),
    ("yzx", 256), ("zyx", 256),
)
RATE = 46.6e3
LATENCY = {1: 2.0, 2: 2.7}


class Event:
    def __init__(self, name, waits, sends, cost, run):
        self.name, self.waits, self.sends, self.cost, self.run = name, waits, sends, cost, run


def in_order(events):
    arrival, free, now, left, done = {}, {}, 0.0, list(events), []
    while left:
        best = None
        for event in left:
            if all(w in arrival for w in event.waits):
                ready = max([arrival[w] for w in event.waits], default=0.0)
                if best is None or ready < best[0]:
                    best = (ready, event)
        ready, event = best
        left.remove(event)
        done.append(event)
        now = max(now, ready) + event.cost
        for key, links, size, hops in event.sends:
            start = max([now] + [free.get(link, 0.0) for link in links])
            for link in links:
                free[link] = start + size / RATE
            arrival[key] = start + size / RATE + LATENCY[hops]
    return done, now


class Plan:
    def __init__(self, here, send_sems, recv_sems):
        self.here, self.send_sems, self.recv_sems = here, send_sems, recv_sems
        self.ids, self.out, self.shape = {}, [], {}

    def index(self, key):
        return self.ids.setdefault(key, len(self.ids))

    def send(self, key, src, dst, device):
        i = self.index(key)
        copy = pltpu.make_async_remote_copy(
            src_ref=src,
            dst_ref=dst,
            send_sem=self.send_sems.at[i],
            recv_sem=self.recv_sems.at[i],
            device_id=device,
            device_id_type=MESH,
        )
        copy.start()
        self.out.append(copy)
        self.shape[key] = copy

    def wait(self, key):
        self.shape[key].wait_recv()


def place():
    dp, mp = lax.axis_index("dp"), lax.axis_index("mp")
    return {"y": dp // 8, "z": lax.rem(dp // 2, 4), "x": lax.rem(dp, 2)}, dp, mp


def moved(at, axis, by):
    to = dict(at)
    to[axis] = lax.rem(at[axis] + by, 2 if axis == "x" else 4)
    return {"dp": (to["y"] * 4 + to["z"]) * 2 + to["x"]}


def rows(start, size):
    return pl.ds(pl.multiple_of(start, 8), size)


def ring_pos(at, axis, by):
    return lax.rem(at[axis] + by, 4)


def chunk_events(tag, order, base, size, at, plan, refs, events):
    diff, out, recv, squares, slot = refs["diff"], refs["out"], refs["recv"], refs["squares"], refs["slot"]
    alloc = refs["alloc"]

    def key(*what):
        return (tag,) + what

    def two(axis):
        return (axis + "+", axis + "-")

    def byte(n):
        return n * 1024

    starts, sizes = [base], [size]
    for axis in order:
        n = 2 if axis == "x" else 4
        sizes.append(sizes[-1] // n)
        starts.append(starts[-1] + at[axis] * sizes[-1])

    def emit(name, waits, sends, cost, run):
        events.append(Event(key(name), waits, sends, cost, run))

    pending = []

    def add_into(start, n, keys):
        def run():
            for k in keys:
                plan.wait(k)
            total = diff[rows(start, n)]
            for k in keys:
                total = total + recv[pl.ds(alloc[k], n)]
            diff[rows(start, n)] = total

        return run

    prepare, waits = refs["load"](base, size), []
    cost = 0.25
    big = True
    for level, axis in enumerate(order):
        start, part = starts[level], sizes[level + 1]
        if axis == "x":
            k = key("rs", level)
            alloc[k] = slot(part)

            def run(prepare=prepare, k=k, start=start, part=part):
                prepare()
                src = rows(start + (1 - at["x"]) * part, part)
                plan.send(k, diff.at[src], recv.at[pl.ds(alloc[k], part)], moved(at, "x", 1))

            emit(("rs", level), waits, [(k, two("x"), byte(part), 2)], cost, run)
            prepare, waits = add_into(starts[level + 1], part, [k]), [k]
        elif big:
            big = False
            half = part // 2
            for k in ("far+", "far-", "in+", "in-", "dep+", "dep-"):
                alloc[key(k)] = slot(half)

            def run(prepare=prepare, axis=axis, start=start, part=part, half=half):
                prepare()
                right, left = moved(at, axis, 1), moved(at, axis, 3)
                p1, p2, p3 = (start + ring_pos(at, axis, i) * part for i in (1, 2, 3))
                for k, src, device in (
                    ("far+", p2, right),
                    ("far-", p2 + half, left),
                    ("in+", p1 + half, right),
                    ("in-", p3, left),
                ):
                    plan.send(key(k), diff.at[rows(src, half)], recv.at[pl.ds(alloc[key(k)], half)], device)

            emit(
                ("rs", level),
                waits,
                [(key(k), (axis + k[-1],), byte(half), 1) for k in ("far+", "far-", "in+", "in-")],
                cost,
                run,
            )
            for sign, by, off in (("+", 1, 0), ("-", 3, half)):

                def run(sign=sign, by=by, off=off, axis=axis, start=start, part=part, half=half):
                    src = start + ring_pos(at, axis, by) * part + off
                    add_into(src, half, [key("far" + sign)])()
                    k = key("dep" + sign)
                    plan.send(
                        k, diff.at[rows(src, half)], recv.at[pl.ds(alloc[k], half)], moved(at, axis, by)
                    )

                emit(
                    "dep" + sign,
                    [key("far" + sign)],
                    [(key("dep" + sign), (axis + sign,), byte(half), 1)],
                    0.05,
                    run,
                )
            first = add_into(starts[level + 1], half, [key("dep+"), key("in-")])
            second = add_into(starts[level + 1] + half, half, [key("in+"), key("dep-")])

            def prepare(first=first, second=second):
                first()
                second()

            waits = [key(k) for k in ("dep+", "in-", "in+", "dep-")]
        else:
            for by in (1, 2, 3):
                alloc[key("rs", level, by)] = slot(part)

            def run(prepare=prepare, axis=axis, start=start, part=part, level=level):
                prepare()
                for by in (1, 3, 2):
                    k = key("rs", level, by)
                    src = start + ring_pos(at, axis, by) * part
                    plan.send(k, diff.at[rows(src, part)], recv.at[pl.ds(alloc[k], part)], moved(at, axis, by))

            emit(
                ("rs", level),
                waits,
                [
                    (key("rs", level, 1), (axis + "+",), byte(part), 1),
                    (key("rs", level, 3), (axis + "-",), byte(part), 1),
                    (key("rs", level, 2), two(axis), byte(part), 2),
                ],
                cost,
                run,
            )
            keys = [key("rs", level, by) for by in (1, 2, 3)]
            prepare, waits = add_into(starts[level + 1], part, keys), keys
        cost = 0.1

    shard, n = starts[3], sizes[3]

    def settle(prepare=prepare):
        prepare()
        total = diff[rows(shard, n)]
        out[rows(shard, n)] = total
        square = total * total
        square = square[:, :128] + square[:, 128:]
        squares[...] += square.reshape(n // 8, 8, 128).sum(axis=0)

    prepare = settle
    refs["settled"].append(waits)
    for level in (2, 1, 0):
        axis = order[level]
        start, part = starts[level + 1], sizes[level + 1]
        if axis == "x":
            k = key("ag", level)

            def run(prepare=prepare, k=k, start=start, part=part):
                prepare()
                plan.send(k, out.at[rows(start, part)], out.at[rows(start, part)], moved(at, "x", 1))

            emit(("ag", level), waits, [(k, two("x"), byte(part), 2)], cost, run)
            waits = [k]
        elif level == (0 if order[0] != "x" else 1):
            half = part // 2

            def run(prepare=prepare, axis=axis, start=start, half=half):
                prepare()
                right, left = moved(at, axis, 1), moved(at, axis, 3)
                for k, src, device in (
                    ("on+", start, right),
                    ("on-", start + half, left),
                    ("end+", start + half, right),
                    ("end-", start, left),
                ):
                    plan.send(key(k), out.at[rows(src, half)], out.at[rows(src, half)], device)

            emit(
                ("ag", level),
                waits,
                [(key(k), (axis + k[-1],), byte(half), 1) for k in ("on+", "on-", "end+", "end-")],
                cost,
                run,
            )
            for sign, by, off in (("+", 1, 0), ("-", 3, half)):

                def run(sign=sign, by=by, off=off, axis=axis, level=level, part=part, half=half):
                    plan.wait(key("on" + sign))
                    src = starts[level] + ring_pos(at, axis, 4 - by) * part + off
                    k = key("last" + sign)
                    plan.send(k, out.at[rows(src, half)], out.at[rows(src, half)], moved(at, axis, by))

                emit(
                    "last" + sign,
                    [key("on" + sign)],
                    [(key("last" + sign), (axis + sign,), byte(half), 1)],
                    0.02,
                    run,
                )
            waits = [key(k) for k in ("end+", "end-", "last+", "last-")]
        else:

            def run(prepare=prepare, axis=axis, start=start, part=part, level=level):
                prepare()
                for by in (1, 3, 2):
                    k = key("ag", level, by)
                    plan.send(k, out.at[rows(start, part)], out.at[rows(start, part)], moved(at, axis, by))

            emit(
                ("ag", level),
                waits,
                [
                    (key("ag", level, 1), (axis + "+",), byte(part), 1),
                    (key("ag", level, 3), (axis + "-",), byte(part), 1),
                    (key("ag", level, 2), two(axis), byte(part), 2),
                ],
                cost,
                run,
            )
            waits = [key("ag", level, by) for by in (1, 2, 3)]
        cost = 0.02

        def prepare(waits=waits):
            for k in waits:
                plan.wait(k)

    emit("end", waits, [], 0.02, prepare)


def norm_events(at, mp, plan, refs, events):
    squares, parts = refs["squares"], refs["parts"]
    waits = [k for keys in refs["settled"] for k in keys]
    waits = list(dict.fromkeys(waits))
    slots = [0]

    def round_of(name, peers, waits, before):
        keys = [("norm", name, i) for i in range(len(peers))]
        base = slots[0]
        slots[0] += len(peers)

        def run():
            before()
            for i, (device, links, hops) in enumerate(peers):
                plan.send(keys[i], squares.at[name], parts.at[base + i], device)

        def after():
            total = squares[name]
            for i, k in enumerate(keys):
                plan.wait(k)
                total = total + parts[base + i]
            squares[name + 1] = total

        sends = [(k, links, 4096, hops) for k, (_, links, hops) in zip(keys, peers)]
        events.append(Event(("norm", name), waits, sends, 0.05, run))
        return keys, after

    def line(axis):
        return [
            (moved(at, axis, 1), (axis + "+",), 1),
            (moved(at, axis, 3), (axis + "-",), 1),
            (moved(at, axis, 2), (axis + "+", axis + "-"), 2),
        ]

    def nothing():
        pass

    keys, after = round_of(0, line("y"), waits, nothing)
    keys, after = round_of(1, line("z"), keys, after)
    peers = []
    for flip in (0, 1):
        for by in range(4):
            if flip or by:
                device = dict(moved(at, "x", flip), mp=lax.rem(mp + by, 4))
                peers.append((device, ("x+", "x-"), 2))
    keys, after = round_of(2, peers, keys, after)
    events.append(Event(("norm", "end"), keys, [], 0.1, after))
    return peers


def kernel(max_norm, count, slow, fast, out, factor, slow_in, fast_in, diff, recv, squares, parts, load_sems, send_sems, recv_sems):
    at, dp, mp = place()
    loads = []
    base = 0
    for i, (_, size) in enumerate(CHUNKS):
        part = pl.ds(base, size)
        for j, (src, dst) in enumerate(((slow, slow_in), (fast, fast_in))):
            copy = pltpu.make_async_copy(src.at[part], dst.at[part], load_sems.at[i, j])
            copy.start()
            loads.append(copy)
        base += size
    squares[...] = jnp.zeros_like(squares)

    plan = Plan(at, send_sems, recv_sems)
    taken = [0]

    def slot(n):
        taken[0] += n
        return taken[0] - n

    def load(base, size):
        index = load.calls
        load.calls += 1

        def run():
            loads[2 * index].wait()
            loads[2 * index + 1].wait()
            part = pl.ds(base, size)
            diff[part] = slow_in[part] - fast_in[part].astype(jnp.float32)

        return run

    load.calls = 0
    refs = {
        "diff": diff, "out": out, "recv": recv, "squares": squares.at[0], "slot": slot,
        "alloc": {}, "load": load, "settled": [],
    }
    events = []
    base = 0
    for i, (order, size) in enumerate(CHUNKS):
        chunk_events(i, order, base, size, at, plan, refs, events)
        base += size
    refs["squares"], refs["parts"] = squares, parts
    peers = norm_events(at, mp, plan, refs, events)
    events, _ = in_order(events)

    barrier = pltpu.get_barrier_semaphore()
    friends = [moved(at, axis, by) for axis in "yz" for by in (1, 2, 3)] + [p[0] for p in peers]
    for device in friends:
        pl.semaphore_signal(barrier, inc=1, device_id=device, device_id_type=MESH)
    pl.semaphore_wait(barrier, len(friends))

    for event in events:
        event.run()
    total = jnp.sum(squares[3], axis=(0, 1), keepdims=True) / (count * count)
    scale = jnp.minimum(1.0, max_norm / (jnp.sqrt(total) + EPSILON)) / count
    factor[...] = jnp.broadcast_to(scale, factor.shape)
    for copy in plan.out:
        copy.wait_send()


def summed(slow, fast, max_norm, count):
    n = slow.shape[0]
    any_space = pl.BlockSpec(memory_space=pl.ANY)
    vmem = pl.BlockSpec(memory_space=pltpu.VMEM)
    f32 = jnp.float32
    return pl.pallas_call(
        lambda *refs: kernel(max_norm, count, *refs),
        out_shape=(jax.ShapeDtypeStruct((n, slow.shape[1]), f32), jax.ShapeDtypeStruct((8, 128), f32)),
        in_specs=[any_space, any_space],
        out_specs=(vmem, vmem),
        scratch_shapes=[
            pltpu.VMEM(slow.shape, f32),
            pltpu.VMEM(fast.shape, fast.dtype),
            pltpu.VMEM(slow.shape, f32),
            pltpu.VMEM((5000, slow.shape[1]), f32),
            pltpu.VMEM((4, 8, 128), f32),
            pltpu.VMEM((13, 8, 128), f32),
            pltpu.SemaphoreType.DMA((len(CHUNKS), 2)),
            pltpu.SemaphoreType.DMA((400,)),
            pltpu.SemaphoreType.DMA((400,)),
        ],
        compiler_params=pltpu.CompilerParams(
            collective_id=0, has_side_effects=True, vmem_limit_bytes=40 * 1024 * 1024
        ),
        name="summed",
    )(slow, fast)


def body(slow_weights, fast_weights, momentum):
    replicas = lax.axis_size("dp")
    entries = slow_weights.shape[0] * slow_weights.shape[1] * slow_weights.shape[2] * lax.axis_size("mp")
    max_norm = CLIP_LEVEL * math.sqrt(entries)
    total, factor = summed(slow_weights[0], fast_weights[0, 0], max_norm, replicas)
    gradient = factor[0, 0] * total[None]
    momentum_next = MOMENTUM_RATE * momentum + gradient
    slow_next = slow_weights - OUTER_RATE * (gradient + MOMENTUM_RATE * momentum_next)
    return (slow_next, momentum_next, slow_next.astype(jnp.bfloat16)[None])


def solution(mesh):
    in_specs = (P(None, None, "mp"), P("dp", None, None, "mp"), P(None, None, "mp"))
    out_specs = (P(None, None, "mp"), P(None, None, "mp"), P("dp", None, None, "mp"))
    return jax.shard_map(body, mesh=mesh, in_specs=in_specs, out_specs=out_specs, check_vma=False)
```

```python
import math

import jax
import jax.numpy as jnp
from jax import lax
from jax.experimental import pallas as pl
from jax.experimental.pallas import tpu as pltpu
from jax.sharding import PartitionSpec as P

MOMENTUM_RATE = 0.9
OUTER_RATE = 0.7
CLIP_LEVEL = 0.2
EPSILON = 1e-06

MESH = pl.DeviceIdType.MESH
LENGTH = {"x": 2, "y": 4, "z": 4}
COLUMNS = 256
Y, Z = ("r:y", "d:zx"), ("r:z", "d:yx")
XY, XZ = ("d:x", "r:y", "d:z"), ("d:x", "r:z", "d:y")
CHUNKS = (
    (XY, 256, 0.0), (Y, 256, 0.0), (Z, 256, 0.0), (XZ, 256, 0.0),
    (Y, 256, 0.0), (Z, 256, 0.0), (XY, 256, 0.0),
    (Y, 256, 0.0), (Z, 256, 0.0), (XZ, 256, 0.0),
    (Y, 256, 0.0), (Z, 256, 0.0),
    (Y, 256, 0.0), (Z, 256, 0.0),
)
LOADS = (768, 1024, 896, 896)
RATE = 46.6e3
HOP = (1.6, 0.6)
ISSUE = 0.03


class Event:
    def __init__(self, waits, run, sends=(), cost=0.02, gives=None, start=0.0):
        self.waits, self.run, self.sends = waits, run, sends
        self.cost, self.gives, self.start = cost, gives, start


def in_order(events):
    arrival, free, now, left, done = {}, {}, 0.0, list(events), []
    need = {}
    for event in events:
        for key, _, _ in event.sends:
            need[key] = need.get(key, 0) + 1
    while left:
        best = None
        for event in left:
            if all(w in arrival and not need.get(w) for w in event.waits):
                ready = max([event.start] + [arrival[w] for w in event.waits])
                if best is None or max(ready, now) < max(best[0], now):
                    best = (ready, event)
        ready, event = best
        left.remove(event)
        done.append(event)
        now = max(now, ready) + event.cost
        for key, size, hops in event.sends:
            now += ISSUE
            end = now
            for axis, by in hops:
                ways = {"y": {1: "+", 3: "-", 2: "+-"}, "z": {1: "+", 3: "-", 2: "+-"}, "x": {1: "+-"}}[axis][by]
                for way in ways:
                    begin = max(now, free.get(axis + way, 0.0))
                    free[axis + way] = begin + size / RATE
                    end = max(end, begin + size / RATE)
            count = sum(2 if axis == "x" else min(by, 4 - by) for axis, by in hops)
            arrival[key] = max(arrival.get(key, 0.0), end + HOP[0] + HOP[1] * count)
            need[key] -= 1
        if event.gives is not None:
            arrival[event.gives] = now
    return done, now


def moved(at, offsets):
    to = dict(at)
    for axis, by in offsets:
        to[axis] = lax.rem(at[axis] + by, LENGTH[axis])
    return {"dp": (to["y"] * 4 + to["z"]) * 2 + to["x"]}


def others(axes):
    found = [()]
    for axis in axes:
        found = [o + ((axis, by),) for o in found for by in range(LENGTH[axis])]
    return [tuple((a, by) for a, by in o if by) for o in found if any(by for _, by in o)]


def rows(start, size):
    return pl.ds(start if isinstance(start, int) else pl.multiple_of(start, 8), size)


class Exchange:
    def __init__(self, recv_sems, send_sems, whole):
        self.recv_sems, self.send_sems, self.whole = recv_sems, send_sems, whole
        self.index, self.size = {}, {}
        self.sent = [0, 0]

    def group(self, key, size):
        self.index.setdefault(key, len(self.index))
        self.size[key] = self.size.get(key, 0) + size

    def send(self, key, src, dst, device, phase):
        pltpu.make_async_remote_copy(
            src_ref=src,
            dst_ref=dst,
            send_sem=self.send_sems.at[phase],
            recv_sem=self.recv_sems.at[self.index[key]],
            device_id=device,
            device_id_type=MESH,
        ).start()

    def wait(self, key):
        part = self.whole.at[pl.ds(0, self.size[key])]
        pltpu.make_async_copy(part, part, self.recv_sems.at[self.index[key]]).wait()

    def drain(self, phase):
        part = self.whole.at[pl.ds(0, self.sent[phase])]
        pltpu.make_async_copy(part, part, self.send_sems.at[phase]).wait()


class Sum:
    def __init__(self, at, exchange, diff, recv, total):
        self.at, self.exchange = at, exchange
        self.diff, self.recv, self.total = diff, recv, total
        self.events, self.settled, self.taken = [], [], 0

    def copy_of(self, key, size, offsets):
        return (key, size * COLUMNS * 4, offsets)

    def expect(self, key, size, phase):
        self.exchange.group(key, size)
        self.exchange.sent[phase] += size

    def slot(self, size):
        self.taken += size
        return self.taken - size

    def add_into(self, start, size, places):
        value = self.diff[rows(start, size)]
        for place in places:
            value = value + self.recv[pl.ds(place, size)]
        self.diff[rows(start, size)] = value

    def scatter(self, key, src, place, size, offsets):
        src_ref, dst_ref = self.diff.at[rows(src, size)], self.recv.at[pl.ds(place, size)]
        self.exchange.send(key, src_ref, dst_ref, moved(self.at, offsets), 0)

    def gather(self, key, start, size, offsets):
        ref = self.total.at[rows(start, size)]
        self.exchange.send(key, ref, ref, moved(self.at, offsets), 1)

    def piece(self, axes, offsets):
        index = 0
        for axis in axes:
            by = dict(offsets).get(axis, 0)
            index = index * LENGTH[axis] + lax.rem(self.at[axis] + by, LENGTH[axis])
        return index

    def chunk(self, tag, levels, base, size, start_time, prepare, square, finish):
        at = self.at
        starts, sizes, kinds = [base], [size], []
        for level in levels:
            kind, axes = level.split(":")
            kinds.append((kind, axes))
            sizes.append(sizes[-1] // math.prod(LENGTH[a] for a in axes))
            starts.append(starts[-1] + self.piece(axes, ()) * sizes[-1])
        waits, cost = [], 0.15
        for i, (kind, axes) in enumerate(kinds):
            args = (tag, i, axes, starts[i], sizes[i + 1], starts[i + 1])
            reduce = self.reduce_ring if kind == "r" else self.reduce_direct
            waits, prepare = reduce(args, waits, prepare, cost, start_time)
            start_time, cost = 0.0, 0.05

        def settle(add=prepare):
            add()
            square(starts[-1], sizes[-1])

        self.settled.append(("settled", tag))
        prepare, gives, stream = settle, ("settled", tag), []
        for i in reversed(range(len(kinds))):
            kind, axes = kinds[i]
            if i == 0 and axes == "x":
                waits, prepare = self.gather_stream(tag, waits, prepare, stream, sizes[1])
                continue
            args = (tag, i, axes, starts[i], sizes[i + 1], starts[i + 1])
            onward = i == 1 and kinds[0][1] == "x"
            build = self.gather_ring if kind == "r" else self.gather_direct
            waits, prepare, stream = build(args, waits, prepare, gives, onward)
            gives = None
        self.events.append(Event(waits, prepare, gives=("end", tag)))
        self.events.append(Event([("end", tag), "factor"], lambda: finish(base, size), cost=0.2))

    def reduce_direct(self, args, waits, prepare, cost, start_time):
        tag, i, axes, start, part, mine = args
        key, offsets = (tag, "rs", i), others(axes)
        places = [self.slot(part) for _ in offsets]
        for _ in offsets:
            self.expect(key, part, 0)

        def run():
            prepare()
            for o, place in zip(offsets, places):
                self.scatter(key, start + self.piece(axes, o) * part, place, part, o)

        sends = [self.copy_of(key, part, o) for o in offsets]
        self.events.append(Event(waits, run, sends, cost, start=start_time))

        def after():
            self.exchange.wait(key)
            self.add_into(mine, part, places)

        return [key], after

    def reduce_ring(self, args, waits, prepare, cost, start_time):
        tag, i, axis, start, part, mine = args
        half = part // 2
        far = {1: (tag, "far+"), 3: (tag, "far-")}
        near = (tag, "near")
        far_at = {1: self.slot(half), 3: self.slot(half)}
        near_at = {(by, h): self.slot(half) for by in (1, 3) for h in (0, 1)}
        for by in (1, 3):
            self.expect(far[by], half, 0)
            self.expect(near, part, 0)

        def quarter(by, h):
            return start + lax.rem(self.at[axis] + by, 4) * part + h * half

        def run():
            prepare()
            for by, h in ((1, 0), (3, 1)):
                self.scatter(far[by], quarter(2, h), far_at[by], half, ((axis, by),))
            for by, h in ((1, 1), (3, 0)):
                self.scatter(near, quarter(by, h), near_at[by, h], half, ((axis, by),))

        sends = [self.copy_of(far[by], half, ((axis, by),)) for by in (1, 3)]
        sends += [self.copy_of(near, half, ((axis, by),)) for by in (1, 3)]
        self.events.append(Event(waits, run, sends, cost, start=start_time))
        for by, h in ((1, 0), (3, 1)):

            def pass_on(by=by, h=h):
                self.exchange.wait(far[by])
                self.add_into(quarter(by, h), half, [far_at[by]])
                self.scatter(near, quarter(by, h), near_at[by, h], half, ((axis, by),))

            self.events.append(Event([far[by]], pass_on, [self.copy_of(near, half, ((axis, by),))], 0.03))

        def after():
            self.exchange.wait(near)
            for h in (0, 1):
                self.add_into(mine + h * half, half, [near_at[1, h], near_at[3, h]])

        return [near], after

    def gather_direct(self, args, waits, prepare, gives, onward):
        tag, i, axes, _, part, mine = args
        key, offsets = (tag, "ag", i), others(axes)
        for _ in offsets:
            self.expect(key, part, 1)

        def run():
            prepare()
            for o in offsets:
                self.gather(key, mine, part, o)

        self.events.append(Event(waits, run, [self.copy_of(key, part, o) for o in offsets], 0.05, gives))
        return [key], lambda: self.exchange.wait(key), None

    def gather_ring(self, args, waits, prepare, gives, onward):
        tag, i, axis, start, part, mine = args
        half = part // 2
        on = {1: (tag, "on+"), 3: (tag, "on-")}
        end, cross = (tag, "end"), (tag, "cross")
        across = (("x", 1),)
        for by in (1, 3):
            self.expect(on[by], half, 1)
            self.expect(end, part, 1)
        if onward:
            self.expect(cross, 4 * part, 1)

        def quarter(by, h):
            return start + lax.rem(self.at[axis] + by, 4) * part + h * half

        def run():
            prepare()
            for by, h in ((1, 0), (3, 1)):
                self.gather(on[by], mine + h * half, half, ((axis, by),))
            for by, h in ((1, 1), (3, 0)):
                self.gather(end, mine + h * half, half, ((axis, by),))
            if onward:
                self.gather(cross, mine, part, across)

        sends = [self.copy_of(on[by], half, ((axis, by),)) for by in (1, 3)]
        sends += [self.copy_of(end, half, ((axis, by),)) for by in (1, 3)]
        sends += [self.copy_of(cross, part, across)] * onward
        self.events.append(Event(waits, run, sends, 0.05, gives))
        for by, h in ((1, 0), (3, 1)):

            def pass_on(by=by, h=h):
                self.exchange.wait(on[by])
                self.gather(end, quarter(4 - by, h), half, ((axis, by),))
                if onward:
                    self.gather(cross, quarter(4 - by, h), half, across)

            sends = [self.copy_of(end, half, ((axis, by),))]
            sends += [self.copy_of(cross, half, across)] * onward
            self.events.append(Event([on[by]], pass_on, sends, 0.03))

        def after():
            self.exchange.wait(end)

        def stream():
            self.gather(cross, quarter(3, 1), half, across)
            self.gather(cross, quarter(1, 0), half, across)
            self.gather(cross, quarter(2, 0), part, across)

        return [end], after, (stream, [half, half, part])

    def gather_stream(self, tag, waits, prepare, stream, size):
        stream, parts = stream
        key = (tag, "cross")

        def run():
            prepare()
            stream()

        self.events.append(Event(waits, run, [self.copy_of(key, n, (("x", 1),)) for n in parts], 0.05))
        return [key], lambda: self.exchange.wait(key)


def norm_events(at, settled, squares, parts, recv_sems, send_sem, finish):
    events, base, friends = [], 0, []
    mp = lax.axis_index("mp")
    rounds = [[(moved(at, o), o) for o in others(axis)] for axis in "yz"]
    last = []
    for flip in (0, 1):
        for by in range(4):
            if flip or by:
                o = (("x", 1),)
                last.append((dict(moved(at, o if flip else ()), mp=lax.rem(mp + by, 4)), o))
    rounds.append(last)
    waits = settled
    for i, peers in enumerate(rounds):
        key, part = ("norm", i), pl.ds(base, len(peers))

        def run(i=i, peers=peers, base=base):
            if i:
                add(i - 1)
            for j, (device, _) in enumerate(peers):
                pltpu.make_async_remote_copy(
                    src_ref=squares.at[i],
                    dst_ref=parts.at[base + j],
                    send_sem=send_sem,
                    recv_sem=recv_sems.at[i],
                    device_id=device,
                    device_id_type=MESH,
                ).start()

        events.append(Event(waits, run, [(key, 4096, o) for _, o in peers], 0.05))
        waits, base = [key], base + len(peers)
        friends += [device for device, _ in peers]

    def add(i):
        start = sum(len(p) for p in rounds[:i])
        n = len(rounds[i])
        part = parts.at[pl.ds(start, n)]
        pltpu.make_async_copy(part, part, recv_sems.at[i]).wait()
        value = squares[i]
        for j in range(n):
            value = value + parts[start + j]
        squares[i + 1] = value

    def end():
        add(2)
        finish()

    events.append(Event(waits, end, cost=0.2, gives="factor"))

    def drain():
        pltpu.make_async_copy(parts, parts, send_sem).wait()

    return events, friends, drain


def kernel(
    max_norm, count, slow, fast, momentum, slow_out, momentum_out, fast_out,
    slow_in, fast_in, momentum_in, diff, recv, total, squares, parts, factor,
    load_sems, recv_sems, send_sems, norm_sems,
):
    dp = lax.axis_index("dp")
    at = {"y": dp // 8, "z": lax.rem(dp // 2, 4), "x": lax.rem(dp, 2)}
    loads, base = [], 0
    for i, size in enumerate(LOADS):
        part = pl.ds(base, size)
        pair = []
        for j, (src, dst) in enumerate(((slow, slow_in), (fast, fast_in))):
            pair.append(pltpu.make_async_copy(src.at[part], dst.at[part], load_sems.at[2 * i + j]))
            pair[-1].start()
        loads.append((base + size, pair))
        base += size
    late = pltpu.make_async_copy(momentum, momentum_in, load_sems.at[2 * len(LOADS)])
    late.start()
    squares[0] = jnp.zeros(squares.shape[1:], squares.dtype)

    def load(base, size):
        def run():
            while loads and (not ready[0] or ready[0] < base + size):
                ready[0], pair = loads.pop(0)
                for copy in pair:
                    copy.wait()
            part = pl.ds(base, size)
            diff[part] = slow_in[part] - fast_in[part].astype(jnp.float32)

        return run

    ready = [0]

    def square(start, size):
        value = diff[rows(start, size)]
        total[rows(start, size)] = value
        value = value * value
        value = value[:, :128] + value[:, 128:]
        squares[0] += value.reshape(size // 8, 8, 128).sum(axis=0)

    def clip():
        norm = jnp.sqrt(jnp.sum(squares[3], axis=(0, 1), keepdims=True)) / count
        scale = jnp.minimum(1.0, max_norm / (norm + EPSILON)) / count
        factor[...] = jnp.broadcast_to(scale, factor.shape)
        late.wait()

    def finish(base, size):
        part = pl.ds(base, size)
        scale = jnp.concatenate([factor[0:1], factor[0:1]], axis=1)
        gradient = scale * total[part]
        momentum_next = MOMENTUM_RATE * momentum_in[part] + gradient
        slow_next = slow_in[part] - OUTER_RATE * (gradient + MOMENTUM_RATE * momentum_next)
        momentum_out[part] = momentum_next
        slow_out[part] = slow_next
        fast_out[part] = slow_next.astype(fast_out.dtype)

    exchange = Exchange(recv_sems, send_sems, total)
    work = Sum(at, exchange, diff, recv, total)
    base = 0
    for tag, (levels, size, start_time) in enumerate(CHUNKS):
        work.chunk(tag, levels, base, size, start_time, load(base, size), square, finish)
        base += size
    events, friends, drain = norm_events(
        at, work.settled, squares, parts, norm_sems, send_sems.at[2], clip
    )
    events, _ = in_order(work.events + events)

    met = {o for o in others("zx") + others("yx")}
    friends = [moved(at, o) for o in sorted(met) if o != (("x", 1),)] + friends[6:]
    barrier = pltpu.get_barrier_semaphore()
    for device in friends:
        pl.semaphore_signal(barrier, inc=1, device_id=device, device_id_type=MESH)
    pl.semaphore_wait(barrier, len(friends))

    for event in events:
        event.run()
    exchange.drain(0)
    exchange.drain(1)
    drain()


def updated(slow, fast, momentum, max_norm, count):
    f32, shape = jnp.float32, slow.shape
    hbm = pl.BlockSpec(memory_space=pltpu.HBM)
    vmem = pl.BlockSpec(memory_space=pltpu.VMEM)
    groups = sum(8 if len(levels) == 2 else 10 for levels, _, _ in CHUNKS)
    return pl.pallas_call(
        lambda *refs: kernel(max_norm, count, *refs),
        out_shape=(pltpu.VMEM(shape, f32), pltpu.VMEM(shape, f32), pltpu.VMEM(shape, fast.dtype)),
        in_specs=[hbm, hbm, hbm],
        out_specs=(vmem, vmem, vmem),
        scratch_shapes=[
            pltpu.VMEM(shape, f32),
            pltpu.VMEM(shape, fast.dtype),
            pltpu.VMEM(shape, f32),
            pltpu.VMEM(shape, f32),
            pltpu.VMEM(shape, f32),
            pltpu.VMEM(shape, f32),
            pltpu.VMEM((4, 8, 128), f32),
            pltpu.VMEM((13, 8, 128), f32),
            pltpu.VMEM((8, 128), f32),
            pltpu.SemaphoreType.DMA((2 * len(LOADS) + 1,)),
            pltpu.SemaphoreType.DMA((groups,)),
            pltpu.SemaphoreType.DMA((3,)),
            pltpu.SemaphoreType.DMA((3,)),
        ],
        compiler_params=pltpu.CompilerParams(
            collective_id=0, has_side_effects=True, vmem_limit_bytes=40 * 1024 * 1024
        ),
        name="updated",
    )(*(pltpu.with_memory_space_constraint(x, pltpu.HBM) for x in (slow, fast, momentum)))


def body(slow_weights, fast_weights, momentum):
    replicas = lax.axis_size("dp")
    entries = slow_weights.shape[0] * slow_weights.shape[1] * slow_weights.shape[2] * lax.axis_size("mp")
    max_norm = CLIP_LEVEL * math.sqrt(entries)
    slow_next, momentum_next, fast_next = updated(
        slow_weights[0], fast_weights[0, 0], momentum[0], max_norm, replicas
    )
    return (slow_next[None], momentum_next[None], fast_next[None, None])


def solution(mesh):
    in_specs = (P(None, None, "mp"), P("dp", None, None, "mp"), P(None, None, "mp"))
    out_specs = (P(None, None, "mp"), P(None, None, "mp"), P("dp", None, None, "mp"))
    return jax.shard_map(body, mesh=mesh, in_specs=in_specs, out_specs=out_specs, check_vma=False)
```

```python
import math

import jax
import jax.numpy as jnp
from jax import lax
from jax.experimental import pallas as pl
from jax.experimental.pallas import tpu as pltpu
from jax.sharding import PartitionSpec as P

MOMENTUM_RATE = 0.9
OUTER_RATE = 0.7
CLIP_LEVEL = 0.2
EPSILON = 1e-06

MESH = pl.DeviceIdType.MESH
LENGTH = {"x": 2, "y": 4, "z": 4}
COLUMNS = 256
Y, Z = ("r:y", "d:zx"), ("r:z", "d:yx")
XY, XZ = ("d:x", "r:y", "d:z"), ("d:x", "r:z", "d:y")
CHUNKS = ((('d:x', 'd:y', 'd:z'), 256, False, ((-1, 21.5),)), (('r:y', 'd:zx'), 256, True, ((-2, 18.3), (-1, 21.4), (0, 1.8), (1, 2.9))), (('d:x', 'd:z', 'd:y'), 256, True, ((-1, 16.4), (0, 1.0), (1, 3.0))), (('r:y', 'd:zx'), 256, True, ((-3, 16.1), (-1, 5.4), (0, 9.9))), (('r:z', 'd:yx'), 256, False, ((-2, 6.7),)), (('r:y', 'd:z', 'd:x'), 256, True, ((-3, 15.6), (-2, 14.7), (-1, 7.1), (1, 9.9))), (('r:z', 'd:yx'), 256, False, ((-3, 5.8), (-2, 21.7), (-1, 0.4), (0, 0), (1, 16.5))), (('d:x', 'r:y', 'd:z'), 256, False, ((-1, 31.0),)), (('r:y', 'd:zx'), 256, True, ((-3, 8.3), (-1, 13.4), (0, 8.0))), (('r:z', 'd:y', 'd:x'), 512, True, ((-1, 23.5),)), (('r:z', 'd:y', 'd:x'), 256, False, ()), (('r:y', 'd:z', 'd:x'), 256, True, ((-3, 3.0), (-2, 4.1), (-1, 17.6), (1, 13.8))), (('d:x', 'd:z', 'd:y'), 256, False, ((-3, 5.2), (0, 6.9), (1, 2.3))))
LOADS = (768, 1024, 896, 896)
RATE = 46.6e3
HOP = (2.1, 0.6)
ISSUE = 0.02


class Event:
    def __init__(self, waits, run, sends=(), cost=0.02, gives=None, start=0.0):
        self.waits, self.run, self.sends = waits, run, sends
        self.cost, self.gives, self.start = cost, gives, start


def in_order(events):
    arrival, free, now, left, done = {}, {}, 0.0, list(events), []
    need = {}
    for event in events:
        for key, _, _ in event.sends:
            need[key] = need.get(key, 0) + 1
    while left:
        best = None
        for event in left:
            if all(w in arrival and not need.get(w) for w in event.waits):
                ready = max([event.start] + [arrival[w] for w in event.waits])
                if best is None or max(ready, now) < max(best[0], now):
                    best = (ready, event)
        ready, event = best
        left.remove(event)
        done.append(event)
        now = max(now, ready) + event.cost
        for key, size, hops in event.sends:
            now += ISSUE
            end = now
            for axis, by in hops:
                ways = {"y": {1: "+", 3: "-", 2: "+-"}, "z": {1: "+", 3: "-", 2: "+-"}, "x": {1: "+-"}}[axis][by]
                for way in ways:
                    begin = max(now, free.get(axis + way, 0.0))
                    free[axis + way] = begin + size / RATE
                    end = max(end, begin + size / RATE)
            count = sum(2 if axis == "x" else min(by, 4 - by) for axis, by in hops)
            arrival[key] = max(arrival.get(key, 0.0), end + HOP[0] + HOP[1] * count)
            need[key] -= 1
        if event.gives is not None:
            arrival[event.gives] = now
    return done, now


def moved(at, offsets):
    to = dict(at)
    for axis, by in offsets:
        to[axis] = lax.rem(at[axis] + by, LENGTH[axis])
    return {"dp": (to["y"] * 4 + to["z"]) * 2 + to["x"]}


def others(axes):
    found = [()]
    for axis in axes:
        found = [o + ((axis, by),) for o in found for by in range(LENGTH[axis])]
    return [tuple((a, by) for a, by in o if by) for o in found if any(by for _, by in o)]


def rows(start, size):
    return pl.ds(start if isinstance(start, int) else pl.multiple_of(start, 8), size)


class Exchange:
    def __init__(self, recv_sems, send_sems, whole):
        self.recv_sems, self.send_sems, self.whole = recv_sems, send_sems, whole
        self.index, self.size = {}, {}
        self.sent = [0, 0]

    def group(self, key, size):
        self.index.setdefault(key, len(self.index))
        self.size[key] = self.size.get(key, 0) + size

    def send(self, key, src, dst, device, phase):
        pltpu.make_async_remote_copy(
            src_ref=src,
            dst_ref=dst,
            send_sem=self.send_sems.at[phase],
            recv_sem=self.recv_sems.at[self.index[key]],
            device_id=device,
            device_id_type=MESH,
        ).start()

    def wait(self, key):
        part = self.whole.at[pl.ds(0, self.size[key])]
        pltpu.make_async_copy(part, part, self.recv_sems.at[self.index[key]]).wait()

    def drain(self, phase):
        part = self.whole.at[pl.ds(0, self.sent[phase])]
        pltpu.make_async_copy(part, part, self.send_sems.at[phase]).wait()


class Sum:
    def __init__(self, at, exchange, diff, recv, total):
        self.at, self.exchange = at, exchange
        self.diff, self.recv, self.total = diff, recv, total
        self.events, self.settled, self.taken = [], [], 0

    def copy_of(self, key, size, offsets):
        return (key, size * COLUMNS * 4, offsets)

    def expect(self, key, size, phase):
        self.exchange.group(key, size)
        self.exchange.sent[phase] += size

    def slot(self, size):
        self.taken += size
        return self.taken - size

    def add_into(self, start, size, places):
        value = self.diff[rows(start, size)]
        for place in places:
            value = value + self.recv[pl.ds(place, size)]
        self.diff[rows(start, size)] = value

    def scatter(self, key, src, place, size, offsets):
        src_ref, dst_ref = self.diff.at[rows(src, size)], self.recv.at[pl.ds(place, size)]
        self.exchange.send(key, src_ref, dst_ref, moved(self.at, offsets), 0)

    def gather(self, key, start, size, offsets):
        ref = self.total.at[rows(start, size)]
        self.exchange.send(key, ref, ref, moved(self.at, offsets), 1)

    def piece(self, axes, offsets):
        index = 0
        for axis in axes:
            by = dict(offsets).get(axis, 0)
            index = index * LENGTH[axis] + lax.rem(self.at[axis] + by, LENGTH[axis])
        return index

    def chunk(self, tag, levels, base, size, early, times, prepare, square, finish):
        self.early = early
        starts, sizes, kinds = [base], [size], []
        for level in levels:
            kind, axes = level.split(":")
            kinds.append((kind, axes))
            sizes.append(sizes[-1] // math.prod(LENGTH[a] for a in axes))
            starts.append(starts[-1] + self.piece(axes, ()) * sizes[-1])
        waits, cost, times = [], 0.15, dict(times)
        for i, (kind, axes) in enumerate(kinds):
            args = (tag, i, axes, starts[i], sizes[i + 1], starts[i + 1])
            reduce = self.reduce_ring if kind == "r" else self.reduce_direct
            waits, prepare = reduce(args, waits, prepare, cost, times.get(i, 0.0))
            cost = 0.05

        def settle(add=prepare):
            add()
            square(starts[-1], sizes[-1])

        self.settled.append(("settled", tag))
        prepare, gives, stream = settle, ("settled", tag), []
        for i in reversed(range(len(kinds))):
            kind, axes = kinds[i]
            if i == 0 and stream:
                waits, prepare = self.gather_stream(tag, waits, prepare, stream, sizes[1])
                continue
            args = (tag, i, axes, starts[i], sizes[i + 1], starts[i + 1])
            onward = i == 1 and kinds[0][1] == "x" and kind == "r"
            build = self.gather_ring if kind == "r" else self.gather_direct
            begun = len(self.events)
            waits, prepare, stream = build(args, waits, prepare, gives, onward)
            self.events[begun].start = times.get(-1 - i, 0.0)
            gives = None
        self.events.append(Event(waits, prepare, gives=("end", tag)))
        self.events.append(Event([("end", tag), "factor"], lambda: finish(base, size), cost=0.2))

    def reduce_direct(self, args, waits, prepare, cost, start_time):
        tag, i, axes, start, part, mine = args
        key, offsets = (tag, "rs", i), others(axes)
        places = [self.slot(part) for _ in offsets]
        for _ in offsets:
            self.expect(key, part, 0)

        def run():
            prepare()
            for o, place in zip(offsets, places):
                self.scatter(key, start + self.piece(axes, o) * part, place, part, o)

        sends = [self.copy_of(key, part, o) for o in offsets]
        self.events.append(Event(waits, run, sends, cost, start=start_time))

        def after():
            self.exchange.wait(key)
            self.add_into(mine, part, places)

        return [key], after

    def reduce_ring(self, args, waits, prepare, cost, start_time):
        tag, i, axis, start, part, mine = args
        half, early = part // 2, self.early
        far = {1: (tag, "far+", i), 3: (tag, "far-", i)}
        near = (tag, "near", i)
        far_at = {1: self.slot(half), 3: self.slot(half)}
        near_at = {(by, h): self.slot(half) for by in (1, 3) for h in (0, 1)}
        for by in (1, 3):
            self.expect(far[by], half, 0)
            self.expect(near, part, 0)

        def quarter(by, h):
            return start + lax.rem(self.at[axis] + by, 4) * part + h * half

        def run():
            prepare()
            for by, h in ((1, 0), (3, 1)):
                self.scatter(far[by], quarter(2, h), far_at[by], half, ((axis, by),))
            if early:
                for by, h in ((1, 1), (3, 0)):
                    self.scatter(near, quarter(by, h), near_at[by, h], half, ((axis, by),))

        sends = [self.copy_of(far[by], half, ((axis, by),)) for by in (1, 3)]
        sends += [self.copy_of(near, half, ((axis, by),)) for by in (1, 3)] * early
        self.events.append(Event(waits, run, sends, cost, start=start_time))
        for by, h in ((1, 0), (3, 1)):

            def pass_on(by=by, h=h):
                self.exchange.wait(far[by])
                self.add_into(quarter(by, h), half, [far_at[by]])
                for k in (h,) if early else (h, 1 - h):
                    self.scatter(near, quarter(by, k), near_at[by, k], half, ((axis, by),))

            sends = [self.copy_of(near, half, ((axis, by),))] * (1 if early else 2)
            self.events.append(Event([far[by]], pass_on, sends, 0.03))

        def after():
            self.exchange.wait(near)
            for h in (0, 1):
                self.add_into(mine + h * half, half, [near_at[1, h], near_at[3, h]])

        return [near], after

    def gather_direct(self, args, waits, prepare, gives, onward):
        tag, i, axes, _, part, mine = args
        key, offsets = (tag, "ag", i), others(axes)
        for _ in offsets:
            self.expect(key, part, 1)

        def run():
            prepare()
            for o in offsets:
                self.gather(key, mine, part, o)

        self.events.append(Event(waits, run, [self.copy_of(key, part, o) for o in offsets], 0.05, gives))
        return [key], lambda: self.exchange.wait(key), None

    def gather_ring(self, args, waits, prepare, gives, onward):
        tag, i, axis, start, part, mine = args
        half = part // 2
        on = {1: (tag, "on+", i), 3: (tag, "on-", i)}
        end, cross = (tag, "end", i), (tag, "cross")
        across = (("x", 1),)
        for by in (1, 3):
            self.expect(on[by], half, 1)
            self.expect(end, part, 1)
        if onward:
            self.expect(cross, 4 * part, 1)

        def quarter(by, h):
            return start + lax.rem(self.at[axis] + by, 4) * part + h * half

        def run():
            prepare()
            for by, h in ((1, 0), (3, 1)):
                self.gather(on[by], mine + h * half, half, ((axis, by),))
            for by, h in ((1, 1), (3, 0)):
                self.gather(end, mine + h * half, half, ((axis, by),))
            if onward:
                self.gather(cross, mine, part, across)

        sends = [self.copy_of(on[by], half, ((axis, by),)) for by in (1, 3)]
        sends += [self.copy_of(end, half, ((axis, by),)) for by in (1, 3)]
        sends += [self.copy_of(cross, part, across)] * onward
        self.events.append(Event(waits, run, sends, 0.05, gives))
        for by, h in ((1, 0), (3, 1)):

            def pass_on(by=by, h=h):
                self.exchange.wait(on[by])
                self.gather(end, quarter(4 - by, h), half, ((axis, by),))
                if onward:
                    self.gather(cross, quarter(4 - by, h), half, across)

            sends = [self.copy_of(end, half, ((axis, by),))]
            sends += [self.copy_of(cross, half, across)] * onward
            self.events.append(Event([on[by]], pass_on, sends, 0.03))

        def after():
            self.exchange.wait(end)

        def stream():
            self.gather(cross, quarter(3, 1), half, across)
            self.gather(cross, quarter(1, 0), half, across)
            self.gather(cross, quarter(2, 0), part, across)

        return [end], after, (stream, [half, half, part]) if onward else None

    def gather_stream(self, tag, waits, prepare, stream, size):
        stream, parts = stream
        key = (tag, "cross")

        def run():
            prepare()
            stream()

        self.events.append(Event(waits, run, [self.copy_of(key, n, (("x", 1),)) for n in parts], 0.05))
        return [key], lambda: self.exchange.wait(key)


def norm_events(at, settled, squares, parts, recv_sems, send_sem, finish):
    events, base, friends = [], 0, []
    mp = lax.axis_index("mp")
    rounds = [[(moved(at, o), o) for o in others("yz")]]
    last = []
    for flip in (0, 1):
        for by in range(4):
            if flip or by:
                o = (("x", 1),)
                last.append((dict(moved(at, o if flip else ()), mp=lax.rem(mp + by, 4)), o))
    rounds.append(last)
    waits = settled
    for i, peers in enumerate(rounds):
        key, part = ("norm", i), pl.ds(base, len(peers))

        def run(i=i, peers=peers, base=base):
            if i:
                add(i - 1)
            for j, (device, _) in enumerate(peers):
                pltpu.make_async_remote_copy(
                    src_ref=squares.at[i],
                    dst_ref=parts.at[base + j],
                    send_sem=send_sem,
                    recv_sem=recv_sems.at[i],
                    device_id=device,
                    device_id_type=MESH,
                ).start()

        events.append(Event(waits, run, [(key, 4096, o) for _, o in peers], 0.05))
        waits, base = [key], base + len(peers)
        friends += [device for device, _ in peers]

    def add(i):
        start = sum(len(p) for p in rounds[:i])
        n = len(rounds[i])
        part = parts.at[pl.ds(start, n)]
        pltpu.make_async_copy(part, part, recv_sems.at[i]).wait()
        value = squares[i]
        for j in range(n):
            value = value + parts[start + j]
        squares[i + 1] = value

    def end():
        add(1)
        finish()

    events.append(Event(waits, end, cost=0.2, gives="factor"))

    def drain():
        pltpu.make_async_copy(parts, parts, send_sem).wait()

    return events, friends, drain


def kernel(
    max_norm, count, slow, fast, momentum, slow_out, momentum_out, fast_out,
    slow_in, fast_in, momentum_in, diff, recv, total, squares, parts, factor,
    load_sems, recv_sems, send_sems, norm_sems,
):
    dp = lax.axis_index("dp")
    at = {"y": dp // 8, "z": lax.rem(dp // 2, 4), "x": lax.rem(dp, 2)}
    loads, base = [], 0
    for i, size in enumerate(LOADS):
        part = pl.ds(base, size)
        pair = []
        for j, (src, dst) in enumerate(((slow, slow_in), (fast, fast_in))):
            pair.append(pltpu.make_async_copy(src.at[part], dst.at[part], load_sems.at[2 * i + j]))
            pair[-1].start()
        loads.append((base + size, pair))
        base += size
    late = pltpu.make_async_copy(momentum, momentum_in, load_sems.at[2 * len(LOADS)])
    late.start()
    squares[0] = jnp.zeros(squares.shape[1:], squares.dtype)

    def load(base, size):
        def run():
            while loads and (not ready[0] or ready[0] < base + size):
                ready[0], pair = loads.pop(0)
                for copy in pair:
                    copy.wait()
            part = pl.ds(base, size)
            diff[part] = slow_in[part] - fast_in[part].astype(jnp.float32)

        return run

    ready = [0]

    def square(start, size):
        value = diff[rows(start, size)]
        total[rows(start, size)] = value
        value = value * value
        value = value[:, :128] + value[:, 128:]
        squares[0] += value.reshape(size // 8, 8, 128).sum(axis=0)

    def clip():
        norm = jnp.sqrt(jnp.sum(squares[2], axis=(0, 1), keepdims=True)) / count
        scale = jnp.minimum(1.0, max_norm / (norm + EPSILON)) / count
        factor[...] = jnp.broadcast_to(scale, factor.shape)
        late.wait()

    def finish(base, size):
        part = pl.ds(base, size)
        scale = jnp.concatenate([factor[0:1], factor[0:1]], axis=1)
        gradient = scale * total[part]
        momentum_next = MOMENTUM_RATE * momentum_in[part] + gradient
        slow_next = slow_in[part] - OUTER_RATE * (gradient + MOMENTUM_RATE * momentum_next)
        momentum_out[part] = momentum_next
        slow_out[part] = slow_next
        fast_out[part] = slow_next.astype(fast_out.dtype)

    exchange = Exchange(recv_sems, send_sems, total)
    work = Sum(at, exchange, diff, recv, total)
    base = 0
    for tag, (levels, size, early, times) in enumerate(CHUNKS):
        work.chunk(tag, levels, base, size, early, times, load(base, size), square, finish)
        base += size
    events, friends, drain = norm_events(
        at, work.settled, squares, parts, norm_sems, send_sems.at[2], clip
    )
    events, _ = in_order(work.events + events)

    friends += [moved(at, o) for o in others("yzx") if o[-1][0] == "x" and len(o) > 1]
    barrier = pltpu.get_barrier_semaphore()
    for device in friends:
        pl.semaphore_signal(barrier, inc=1, device_id=device, device_id_type=MESH)
    pl.semaphore_wait(barrier, len(friends))

    for event in events:
        event.run()
    exchange.drain(0)
    exchange.drain(1)
    drain()


def updated(slow, fast, momentum, max_norm, count):
    f32, shape = jnp.float32, slow.shape
    hbm = pl.BlockSpec(memory_space=pltpu.HBM)
    vmem = pl.BlockSpec(memory_space=pltpu.VMEM)
    groups = sum(2 if level[0] == "d" else 6 for chunk in CHUNKS for level in chunk[0])
    return pl.pallas_call(
        lambda *refs: kernel(max_norm, count, *refs),
        out_shape=(pltpu.VMEM(shape, f32), pltpu.VMEM(shape, f32), pltpu.VMEM(shape, fast.dtype)),
        in_specs=[hbm, hbm, hbm],
        out_specs=(vmem, vmem, vmem),
        scratch_shapes=[
            pltpu.VMEM(shape, f32),
            pltpu.VMEM(shape, fast.dtype),
            pltpu.VMEM(shape, f32),
            pltpu.VMEM(shape, f32),
            pltpu.VMEM(shape, f32),
            pltpu.VMEM(shape, f32),
            pltpu.VMEM((3, 8, 128), f32),
            pltpu.VMEM((22, 8, 128), f32),
            pltpu.VMEM((8, 128), f32),
            pltpu.SemaphoreType.DMA((2 * len(LOADS) + 1,)),
            pltpu.SemaphoreType.DMA((groups,)),
            pltpu.SemaphoreType.DMA((3,)),
            pltpu.SemaphoreType.DMA((2,)),
        ],
        compiler_params=pltpu.CompilerParams(
            collective_id=0, has_side_effects=True, vmem_limit_bytes=40 * 1024 * 1024
        ),
        name="updated",
    )(*(pltpu.with_memory_space_constraint(x, pltpu.HBM) for x in (slow, fast, momentum)))


def written(*values):
    def run(*refs):
        n = len(values)
        copies = [pltpu.make_async_copy(refs[i], refs[n + i], refs[-1].at[i]) for i in range(n)]
        for copy in copies:
            copy.start()
        for copy in copies:
            copy.wait()

    return pl.pallas_call(
        run,
        out_shape=tuple(pltpu.HBM(x.shape, x.dtype) for x in values),
        in_specs=[pl.BlockSpec(memory_space=pltpu.VMEM)] * len(values),
        out_specs=tuple(pl.BlockSpec(memory_space=pltpu.HBM) for _ in values),
        scratch_shapes=[pltpu.SemaphoreType.DMA((len(values),))],
        compiler_params=pltpu.CompilerParams(vmem_limit_bytes=1024 * 1024),
        name="written",
    )(*(pltpu.with_memory_space_constraint(x, pltpu.VMEM) for x in values))


def body(slow_weights, fast_weights, momentum):
    replicas = lax.axis_size("dp")
    entries = slow_weights.shape[0] * slow_weights.shape[1] * slow_weights.shape[2] * lax.axis_size("mp")
    max_norm = CLIP_LEVEL * math.sqrt(entries)
    values = updated(slow_weights[0], fast_weights[0, 0], momentum[0], max_norm, replicas)
    slow_next, momentum_next, fast_next = written(*values)
    return (slow_next[None], momentum_next[None], fast_next[None, None])


def solution(mesh):
    in_specs = (P(None, None, "mp"), P("dp", None, None, "mp"), P(None, None, "mp"))
    out_specs = (P(None, None, "mp"), P(None, None, "mp"), P("dp", None, None, "mp"))
    return jax.shard_map(body, mesh=mesh, in_specs=in_specs, out_specs=out_specs, check_vma=False)
```

```python
import math

import jax
import jax.numpy as jnp
from jax import lax
from jax.experimental import pallas as pl
from jax.experimental.pallas import tpu as pltpu
from jax.sharding import PartitionSpec as P

MOMENTUM_RATE = 0.9
OUTER_RATE = 0.7
CLIP_LEVEL = 0.2
EPSILON = 1e-06

MESH = pl.DeviceIdType.MESH
LENGTH = {"x": 2, "y": 4, "z": 4}
COLUMNS = 256
Y, Z = ("r:y", "d:zx"), ("r:z", "d:yx")
XY, XZ = ("d:x", "r:y", "d:z"), ("d:x", "r:z", "d:y")
CHUNKS = ((('r:z', 'd:x', 'd:y'), 256, False, ((-3, 3.8), (-2, 21.5), (-1, 5.5))), (('r:y', 'd:zx'), 256, True, ((-3, 0), (-1, 24.3), (0, 2.4))), (('r:y', 'd:x', 'd:z'), 256, False, ((-3, 7.3), (-2, 20.8), (-1, 24.4), (1, 2.7))), (('r:z', 'd:x', 'd:y'), 256, False, ((-3, 17.4), (-2, 11.1), (-1, 16.4), (1, 1.7))), (('r:y', 'd:zx'), 256, True, ((-3, 25.2), (-2, 3.6), (-1, 14.7), (1, 9.6))), (('d:x', 'r:z', 'd:y'), 256, False, ((-3, 1.7), (-1, 14.7), (1, 1.0))), (('r:y', 'd:zx'), 256, False, ((-3, 21.7), (-2, 18.7), (-1, 15.2), (1, 10.1))), (('r:z', 'd:x', 'd:y'), 256, True, ((-3, 20.1), (-2, 0), (-1, 5.5))), (('r:z', 'd:yx'), 256, True, ((-2, 12.5), (-1, 13.4), (0, 1.3), (1, 14.0))), (('d:x', 'd:y', 'd:z'), 256, True, ((-3, 5.6), (-1, 13.5), (0, 3.2), (1, 0.2))), (('r:y', 'd:zx'), 256, True, ((-2, 10.2), (-1, 4.9), (0, 5.1), (1, 11.6))), (('r:y', 'd:zx'), 256, True, ((-2, 0), (-1, 12.0))), (('r:z', 'd:x', 'd:y'), 256, True, ((-1, 20.7),)), (('d:x', 'd:z', 'd:y'), 256, False, ((-3, 5.2),)))
LOADS = (512, 768, 1024, 1280)
RATE = 45e3
HOP = (2.7, 0.5)
ISSUE = 0.01
COST = 0.4


class Event:
    def __init__(self, waits, run, sends=(), cost=0.02, gives=None, start=0.0):
        self.waits, self.run, self.sends = waits, run, sends
        self.cost, self.gives, self.start = cost, gives, start


def in_order(events):
    arrival, free, now, left, done = {}, {}, 0.0, list(events), []
    need = {}
    for event in events:
        for key, _, _ in event.sends:
            need[key] = need.get(key, 0) + 1
    while left:
        best = None
        for event in left:
            if all(w in arrival and not need.get(w) for w in event.waits):
                ready = max([event.start] + [arrival[w] for w in event.waits])
                if best is None or max(ready, now) < max(best[0], now):
                    best = (ready, event)
        ready, event = best
        left.remove(event)
        done.append(event)
        now = max(now, ready) + COST * event.cost
        for key, size, hops in event.sends:
            now += ISSUE
            end = now
            for axis, by in hops:
                ways = {"y": {1: "+", 3: "-", 2: "+-"}, "z": {1: "+", 3: "-", 2: "+-"}, "x": {1: "+-"}}[axis][by]
                for way in ways:
                    begin = max(now, free.get(axis + way, 0.0))
                    free[axis + way] = begin + size / RATE
                    end = max(end, begin + size / RATE)
            count = sum(2 if axis == "x" else min(by, 4 - by) for axis, by in hops)
            arrival[key] = max(arrival.get(key, 0.0), end + HOP[0] + HOP[1] * count)
            need[key] -= 1
        if event.gives is not None:
            arrival[event.gives] = now
    return done, now


def moved(at, offsets):
    to = dict(at)
    for axis, by in offsets:
        to[axis] = lax.rem(at[axis] + by, LENGTH[axis])
    return {"dp": (to["y"] * 4 + to["z"]) * 2 + to["x"]}


def others(axes):
    found = [()]
    for axis in axes:
        found = [o + ((axis, by),) for o in found for by in range(LENGTH[axis])]
    return [tuple((a, by) for a, by in o if by) for o in found if any(by for _, by in o)]


def rows(start, size):
    return pl.ds(start if isinstance(start, int) else pl.multiple_of(start, 8), size)


class Exchange:
    def __init__(self, recv_sems, send_sems, whole):
        self.recv_sems, self.send_sems, self.whole = recv_sems, send_sems, whole
        self.index, self.size = {}, {}
        self.sent = [0, 0]

    def group(self, key, size):
        self.index.setdefault(key, len(self.index))
        self.size[key] = self.size.get(key, 0) + size

    def send(self, key, src, dst, device, phase):
        pltpu.make_async_remote_copy(
            src_ref=src,
            dst_ref=dst,
            send_sem=self.send_sems.at[phase],
            recv_sem=self.recv_sems.at[self.index[key]],
            device_id=device,
            device_id_type=MESH,
        ).start()

    def wait(self, key):
        part = self.whole.at[pl.ds(0, self.size[key])]
        pltpu.make_async_copy(part, part, self.recv_sems.at[self.index[key]]).wait()

    def drain(self, phase):
        part = self.whole.at[pl.ds(0, self.sent[phase])]
        pltpu.make_async_copy(part, part, self.send_sems.at[phase]).wait()


class Sum:
    def __init__(self, at, exchange, diff, recv, total):
        self.at, self.exchange = at, exchange
        self.diff, self.recv, self.total = diff, recv, total
        self.events, self.settled, self.taken = [], [], 0

    def copy_of(self, key, size, offsets):
        return (key, size * COLUMNS * 4, offsets)

    def expect(self, key, size, phase):
        self.exchange.group(key, size)
        self.exchange.sent[phase] += size

    def slot(self, size):
        self.taken += size
        return self.taken - size

    def add_into(self, start, size, places):
        value = self.diff[rows(start, size)]
        for place in places:
            value = value + self.recv[pl.ds(place, size)]
        self.diff[rows(start, size)] = value

    def scatter(self, key, src, place, size, offsets):
        src_ref, dst_ref = self.diff.at[rows(src, size)], self.recv.at[pl.ds(place, size)]
        self.exchange.send(key, src_ref, dst_ref, moved(self.at, offsets), 0)

    def gather(self, key, start, size, offsets):
        ref = self.total.at[rows(start, size)]
        self.exchange.send(key, ref, ref, moved(self.at, offsets), 1)

    def piece(self, axes, offsets):
        index = 0
        for axis in axes:
            by = dict(offsets).get(axis, 0)
            index = index * LENGTH[axis] + lax.rem(self.at[axis] + by, LENGTH[axis])
        return index

    def chunk(self, tag, levels, base, size, early, times, prepare, square, finish):
        self.early = early
        starts, sizes, kinds = [base], [size], []
        for level in levels:
            kind, axes = level.split(":")
            kinds.append((kind, axes))
            sizes.append(sizes[-1] // math.prod(LENGTH[a] for a in axes))
            starts.append(starts[-1] + self.piece(axes, ()) * sizes[-1])
        waits, cost, times = [], 0.15, dict(times)
        for i, (kind, axes) in enumerate(kinds):
            args = (tag, i, axes, starts[i], sizes[i + 1], starts[i + 1])
            reduce = self.reduce_ring if kind == "r" else self.reduce_direct
            waits, prepare = reduce(args, waits, prepare, cost, times.get(i, 0.0))
            cost = 0.05

        def settle(add=prepare):
            add()
            square(starts[-1], sizes[-1])

        self.settled.append(("settled", tag))
        prepare, gives, stream = settle, ("settled", tag), []
        for i in reversed(range(len(kinds))):
            kind, axes = kinds[i]
            if i == 0 and stream:
                waits, prepare = self.gather_stream(tag, waits, prepare, stream, sizes[1])
                continue
            args = (tag, i, axes, starts[i], sizes[i + 1], starts[i + 1])
            onward = i == 1 and kinds[0][1] == "x" and kind == "r"
            build = self.gather_ring if kind == "r" else self.gather_direct
            begun = len(self.events)
            waits, prepare, stream = build(args, waits, prepare, gives, onward)
            self.events[begun].start = times.get(-1 - i, 0.0)
            gives = None
        self.events.append(Event(waits, prepare, gives=("end", tag)))
        self.events.append(Event([("end", tag), "factor"], lambda: finish(base, size), cost=0.2))

    def reduce_direct(self, args, waits, prepare, cost, start_time):
        tag, i, axes, start, part, mine = args
        key, offsets = (tag, "rs", i), others(axes)
        places = [self.slot(part) for _ in offsets]
        for _ in offsets:
            self.expect(key, part, 0)

        def run():
            prepare()
            for o, place in zip(offsets, places):
                self.scatter(key, start + self.piece(axes, o) * part, place, part, o)

        sends = [self.copy_of(key, part, o) for o in offsets]
        self.events.append(Event(waits, run, sends, cost, start=start_time))

        def after():
            self.exchange.wait(key)
            self.add_into(mine, part, places)

        return [key], after

    def reduce_ring(self, args, waits, prepare, cost, start_time):
        tag, i, axis, start, part, mine = args
        half, early = part // 2, self.early
        far = (tag, "far", i)
        near = (tag, "near", i)
        far_at = {1: self.slot(half), 3: self.slot(half)}
        near_at = {(by, h): self.slot(half) for by in (1, 3) for h in (0, 1)}
        for by in (1, 3):
            self.expect(far, half, 0)
            self.expect(near, part, 0)

        def quarter(by, h):
            return start + lax.rem(self.at[axis] + by, 4) * part + h * half

        def run():
            prepare()
            for by, h in ((1, 0), (3, 1)):
                self.scatter(far, quarter(2, h), far_at[by], half, ((axis, by),))
            if early:
                for by, h in ((1, 1), (3, 0)):
                    self.scatter(near, quarter(by, h), near_at[by, h], half, ((axis, by),))

        sends = [self.copy_of(far, half, ((axis, by),)) for by in (1, 3)]
        sends += [self.copy_of(near, half, ((axis, by),)) for by in (1, 3)] * early
        self.events.append(Event(waits, run, sends, cost, start=start_time))

        def pass_on():
            self.exchange.wait(far)
            for by, h in ((1, 0), (3, 1)):
                self.add_into(quarter(by, h), half, [far_at[by]])
            for by, h in ((1, 0), (3, 1)) if early else ((1, 0), (3, 1), (1, 1), (3, 0)):
                self.scatter(near, quarter(by, h), near_at[by, h], half, ((axis, by),))

        sends = [self.copy_of(near, half, ((axis, by),)) for by in (1, 3)]
        self.events.append(Event([far], pass_on, sends * (1 if early else 2), 0.06))

        def after():
            self.exchange.wait(near)
            for h in (0, 1):
                self.add_into(mine + h * half, half, [near_at[1, h], near_at[3, h]])

        return [near], after

    def gather_direct(self, args, waits, prepare, gives, onward):
        tag, i, axes, _, part, mine = args
        key, offsets = (tag, "ag", i), others(axes)
        for _ in offsets:
            self.expect(key, part, 1)

        def run():
            prepare()
            for o in offsets:
                self.gather(key, mine, part, o)

        self.events.append(Event(waits, run, [self.copy_of(key, part, o) for o in offsets], 0.05, gives))
        return [key], lambda: self.exchange.wait(key), None

    def gather_ring(self, args, waits, prepare, gives, onward):
        tag, i, axis, start, part, mine = args
        half = part // 2
        on = (tag, "on", i)
        end, cross = (tag, "end", i), (tag, "cross")
        across = (("x", 1),)
        for by in (1, 3):
            self.expect(on, half, 1)
            self.expect(end, part, 1)
        if onward:
            self.expect(cross, 4 * part, 1)

        def quarter(by, h):
            return start + lax.rem(self.at[axis] + by, 4) * part + h * half

        def run():
            prepare()
            for by, h in ((1, 0), (3, 1)):
                self.gather(on, mine + h * half, half, ((axis, by),))
            for by, h in ((1, 1), (3, 0)):
                self.gather(end, mine + h * half, half, ((axis, by),))
            if onward:
                self.gather(cross, mine, part, across)

        sends = [self.copy_of(on, half, ((axis, by),)) for by in (1, 3)]
        sends += [self.copy_of(end, half, ((axis, by),)) for by in (1, 3)]
        sends += [self.copy_of(cross, part, across)] * onward
        self.events.append(Event(waits, run, sends, 0.05, gives))

        def pass_on():
            self.exchange.wait(on)
            for by, h in ((1, 0), (3, 1)):
                self.gather(end, quarter(4 - by, h), half, ((axis, by),))
            if onward:
                for by, h in ((1, 0), (3, 1)):
                    self.gather(cross, quarter(4 - by, h), half, across)

        sends = [self.copy_of(end, half, ((axis, by),)) for by in (1, 3)]
        sends += [self.copy_of(cross, half, across)] * (2 * onward)
        self.events.append(Event([on], pass_on, sends, 0.03))

        def after():
            self.exchange.wait(end)

        def stream():
            self.gather(cross, quarter(3, 1), half, across)
            self.gather(cross, quarter(1, 0), half, across)
            self.gather(cross, quarter(2, 0), part, across)

        return [end], after, (stream, [half, half, part]) if onward else None

    def gather_stream(self, tag, waits, prepare, stream, size):
        stream, parts = stream
        key = (tag, "cross")

        def run():
            prepare()
            stream()

        self.events.append(Event(waits, run, [self.copy_of(key, n, (("x", 1),)) for n in parts], 0.05))
        return [key], lambda: self.exchange.wait(key)


def norm_events(at, settled, squares, parts, recv_sems, send_sem, finish):
    events, base, friends = [], 0, []
    mp = lax.axis_index("mp")
    rounds = [[(moved(at, o), o) for o in others("yz")]]
    last = []
    for flip in (0, 1):
        for by in range(4):
            if flip or by:
                o = (("x", 1),)
                last.append((dict(moved(at, o if flip else ()), mp=lax.rem(mp + by, 4)), o))
    rounds.append(last)
    waits = settled
    for i, peers in enumerate(rounds):
        key, part = ("norm", i), pl.ds(base, len(peers))

        def run(i=i, peers=peers, base=base):
            if i:
                add(i - 1)
            for j, (device, _) in enumerate(peers):
                pltpu.make_async_remote_copy(
                    src_ref=squares.at[i],
                    dst_ref=parts.at[base + j],
                    send_sem=send_sem,
                    recv_sem=recv_sems.at[i],
                    device_id=device,
                    device_id_type=MESH,
                ).start()

        events.append(Event(waits, run, [(key, 4096, o) for _, o in peers], 0.05))
        waits, base = [key], base + len(peers)
        friends += [device for device, _ in peers]

    def add(i):
        start = sum(len(p) for p in rounds[:i])
        n = len(rounds[i])
        part = parts.at[pl.ds(start, n)]
        pltpu.make_async_copy(part, part, recv_sems.at[i]).wait()
        value = squares[i]
        for j in range(n):
            value = value + parts[start + j]
        squares[i + 1] = value

    def end():
        add(1)
        finish()

    events.append(Event(waits, end, cost=0.2, gives="factor"))

    def drain():
        pltpu.make_async_copy(parts, parts, send_sem).wait()

    return events, friends, drain


def kernel(
    max_norm, count, slow, fast, momentum, slow_out, momentum_out, fast_out,
    slow_in, fast_in, momentum_in, diff, recv, total, squares, parts, factor,
    load_sems, recv_sems, send_sems, norm_sems,
):
    dp = lax.axis_index("dp")
    at = {"y": dp // 8, "z": lax.rem(dp // 2, 4), "x": lax.rem(dp, 2)}
    loads, base = [], 0
    for i, size in enumerate(LOADS):
        part = pl.ds(base, size)
        pair = []
        for j, (src, dst) in enumerate(((slow, slow_in), (fast, fast_in))):
            pair.append(pltpu.make_async_copy(src.at[part], dst.at[part], load_sems.at[2 * i + j]))
            pair[-1].start()
        loads.append((base + size, pair))
        base += size
    late = pltpu.make_async_copy(momentum, momentum_in, load_sems.at[2 * len(LOADS)])
    squares[0] = jnp.zeros(squares.shape[1:], squares.dtype)

    def load(base, size):
        def run():
            while loads and (not ready[0] or ready[0] < base + size):
                ready[0], pair = loads.pop(0)
                for copy in pair:
                    copy.wait()
            part = pl.ds(base, size)
            diff[part] = slow_in[part] - fast_in[part].astype(jnp.float32)

        return run

    ready = [0]

    def square(start, size):
        value = diff[rows(start, size)]
        total[rows(start, size)] = value
        value = value * value
        value = value[:, :128] + value[:, 128:]
        squares[0] += value.reshape(size // 8, 8, 128).sum(axis=0)

    def clip():
        norm = jnp.sqrt(jnp.sum(squares[2], axis=(0, 1), keepdims=True)) / count
        scale = jnp.minimum(1.0, max_norm / (norm + EPSILON)) / count
        factor[...] = jnp.broadcast_to(scale, factor.shape)
        late.wait()

    def finish(base, size):
        part = pl.ds(base, size)
        scale = jnp.concatenate([factor[0:1], factor[0:1]], axis=1)
        gradient = scale * total[part]
        momentum_next = MOMENTUM_RATE * momentum_in[part] + gradient
        slow_next = slow_in[part] - OUTER_RATE * (gradient + MOMENTUM_RATE * momentum_next)
        momentum_out[part] = momentum_next
        slow_out[part] = slow_next
        fast_out[part] = slow_next.astype(fast_out.dtype)

    exchange = Exchange(recv_sems, send_sems, total)
    work = Sum(at, exchange, diff, recv, total)
    base = 0
    for tag, (levels, size, early, times) in enumerate(CHUNKS):
        work.chunk(tag, levels, base, size, early, times, load(base, size), square, finish)
        base += size
    events, friends, drain = norm_events(
        at, work.settled, squares, parts, norm_sems, send_sems.at[2], clip
    )
    events, _ = in_order(work.events + events)

    friends += [moved(at, o) for o in others("yzx") if o[-1][0] == "x" and len(o) > 1]
    barrier = pltpu.get_barrier_semaphore()
    for device in friends:
        pl.semaphore_signal(barrier, inc=1, device_id=device, device_id_type=MESH)
    pl.semaphore_wait(barrier, len(friends))

    for i, event in enumerate(events):
        if i == len(CHUNKS):
            late.start()
        event.run()
    exchange.drain(0)
    exchange.drain(1)
    drain()


def updated(slow, fast, momentum, max_norm, count):
    f32, shape = jnp.float32, slow.shape
    hbm = pl.BlockSpec(memory_space=pltpu.HBM)
    vmem = pl.BlockSpec(memory_space=pltpu.VMEM)
    groups = sum(2 if level[0] == "d" else 4 for chunk in CHUNKS for level in chunk[0])
    return pl.pallas_call(
        lambda *refs: kernel(max_norm, count, *refs),
        out_shape=(pltpu.VMEM(shape, f32), pltpu.VMEM(shape, f32), pltpu.VMEM(shape, fast.dtype)),
        in_specs=[hbm, hbm, hbm],
        out_specs=(vmem, vmem, vmem),
        scratch_shapes=[
            pltpu.VMEM(shape, f32),
            pltpu.VMEM(shape, fast.dtype),
            pltpu.VMEM(shape, f32),
            pltpu.VMEM(shape, f32),
            pltpu.VMEM(shape, f32),
            pltpu.VMEM(shape, f32),
            pltpu.VMEM((3, 8, 128), f32),
            pltpu.VMEM((22, 8, 128), f32),
            pltpu.VMEM((8, 128), f32),
            pltpu.SemaphoreType.DMA((2 * len(LOADS) + 1,)),
            pltpu.SemaphoreType.DMA((groups,)),
            pltpu.SemaphoreType.DMA((3,)),
            pltpu.SemaphoreType.DMA((2,)),
        ],
        compiler_params=pltpu.CompilerParams(
            collective_id=0, has_side_effects=True, vmem_limit_bytes=40 * 1024 * 1024
        ),
        name="updated",
    )(*(pltpu.with_memory_space_constraint(x, pltpu.HBM) for x in (slow, fast, momentum)))


def written(*values):
    def run(*refs):
        n = len(values)
        copies = [pltpu.make_async_copy(refs[i], refs[n + i], refs[-1].at[i]) for i in range(n)]
        for copy in copies:
            copy.start()
        for copy in copies:
            copy.wait()

    return pl.pallas_call(
        run,
        out_shape=tuple(pltpu.HBM(x.shape, x.dtype) for x in values),
        in_specs=[pl.BlockSpec(memory_space=pltpu.VMEM)] * len(values),
        out_specs=tuple(pl.BlockSpec(memory_space=pltpu.HBM) for _ in values),
        scratch_shapes=[pltpu.SemaphoreType.DMA((len(values),))],
        compiler_params=pltpu.CompilerParams(vmem_limit_bytes=1024 * 1024),
        name="written",
    )(*(pltpu.with_memory_space_constraint(x, pltpu.VMEM) for x in values))


def body(slow_weights, fast_weights, momentum):
    replicas = lax.axis_size("dp")
    entries = slow_weights.shape[0] * slow_weights.shape[1] * slow_weights.shape[2] * lax.axis_size("mp")
    max_norm = CLIP_LEVEL * math.sqrt(entries)
    values = updated(slow_weights[0], fast_weights[0, 0], momentum[0], max_norm, replicas)
    slow_next, momentum_next, fast_next = written(*values)
    return (slow_next[None], momentum_next[None], fast_next[None, None])


def solution(mesh):
    in_specs = (P(None, None, "mp"), P("dp", None, None, "mp"), P(None, None, "mp"))
    out_specs = (P(None, None, "mp"), P(None, None, "mp"), P("dp", None, None, "mp"))
    return jax.shard_map(body, mesh=mesh, in_specs=in_specs, out_specs=out_specs, check_vma=False)
```

```python
import math

import jax
import jax.numpy as jnp
from jax import lax
from jax.experimental import pallas as pl
from jax.experimental.pallas import tpu as pltpu
from jax.sharding import PartitionSpec as P

MOMENTUM_RATE = 0.9
OUTER_RATE = 0.7
CLIP_LEVEL = 0.2
EPSILON = 1e-06

MESH = pl.DeviceIdType.MESH
LENGTH = {"x": 2, "y": 4, "z": 4}
COLUMNS = 256
Y, Z = ("r:y", "d:zx"), ("r:z", "d:yx")
XY, XZ = ("d:x", "r:y", "d:z"), ("d:x", "r:z", "d:y")
CHUNKS = ((('r:z', 'd:x', 'd:y'), 256, False, ((-3, 3.8), (-2, 21.5), (-1, 5.5))), (('r:y', 'd:zx'), 256, True, ((-3, 0), (-1, 24.3), (0, 2.4))), (('r:y', 'd:x', 'd:z'), 256, False, ((-3, 7.3), (-2, 20.8), (-1, 24.4), (1, 2.7))), (('r:z', 'd:x', 'd:y'), 256, False, ((-3, 17.4), (-2, 11.1), (-1, 16.4), (1, 1.7))), (('r:y', 'd:zx'), 256, True, ((-3, 25.2), (-2, 3.6), (-1, 14.7), (1, 9.6))), (('d:x', 'r:z', 'd:y'), 256, False, ((-3, 1.7), (-1, 14.7), (1, 1.0))), (('r:y', 'd:zx'), 256, False, ((-3, 21.7), (-2, 18.7), (-1, 15.2), (1, 10.1))), (('r:z', 'd:x', 'd:y'), 256, True, ((-3, 20.1), (-2, 0), (-1, 5.5))), (('r:z', 'd:yx'), 256, True, ((-2, 12.5), (-1, 13.4), (0, 1.3), (1, 14.0))), (('d:x', 'd:y', 'd:z'), 256, True, ((-3, 5.6), (-1, 13.5), (0, 3.2), (1, 0.2))), (('r:y', 'd:zx'), 256, True, ((-2, 10.2), (-1, 4.9), (0, 5.1), (1, 11.6))), (('r:y', 'd:zx'), 256, True, ((-2, 0), (-1, 12.0))), (('r:z', 'd:x', 'd:y'), 256, True, ((-1, 20.7),)), (('d:x', 'd:z', 'd:y'), 256, False, ((-3, 5.2),)))
LOADS = (512, 768, 1024, 1280)
RATE = 45e3
HOP = (2.7, 0.5)
ISSUE = 0.01
COST = 0.4


class Event:
    def __init__(self, waits, run, sends=(), cost=0.02, gives=None, start=0.0):
        self.waits, self.run, self.sends = waits, run, sends
        self.cost, self.gives, self.start = cost, gives, start


def in_order(events):
    arrival, free, now, left, done = {}, {}, 0.0, list(events), []
    need = {}
    for event in events:
        for key, _, _ in event.sends:
            need[key] = need.get(key, 0) + 1
    while left:
        best = None
        for event in left:
            if all(w in arrival and not need.get(w) for w in event.waits):
                ready = max([event.start] + [arrival[w] for w in event.waits])
                if best is None or max(ready, now) < max(best[0], now):
                    best = (ready, event)
        ready, event = best
        left.remove(event)
        done.append(event)
        now = max(now, ready) + COST * event.cost
        for key, size, hops in event.sends:
            now += ISSUE
            end = now
            for axis, by in hops:
                ways = {"y": {1: "+", 3: "-", 2: "+-"}, "z": {1: "+", 3: "-", 2: "+-"}, "x": {1: "+-"}}[axis][by]
                for way in ways:
                    begin = max(now, free.get(axis + way, 0.0))
                    free[axis + way] = begin + size / RATE
                    end = max(end, begin + size / RATE)
            count = sum(2 if axis == "x" else min(by, 4 - by) for axis, by in hops)
            arrival[key] = max(arrival.get(key, 0.0), end + HOP[0] + HOP[1] * count)
            need[key] -= 1
        if event.gives is not None:
            arrival[event.gives] = now
    return done, now


def moved(at, offsets):
    to = dict(at)
    for axis, by in offsets:
        to[axis] = lax.rem(at[axis] + by, LENGTH[axis])
    return {"dp": (to["y"] * 4 + to["z"]) * 2 + to["x"]}


def others(axes):
    found = [()]
    for axis in axes:
        found = [o + ((axis, by),) for o in found for by in range(LENGTH[axis])]
    return [tuple((a, by) for a, by in o if by) for o in found if any(by for _, by in o)]


def steps(offsets):
    return sum(min(by, LENGTH[axis] - by) for axis, by in offsets)


def rows(start, size):
    return pl.ds(start if isinstance(start, int) else pl.multiple_of(start, 8), size)


class Exchange:
    def __init__(self, recv_sems, send_sems, whole):
        self.recv_sems, self.send_sems, self.whole = recv_sems, send_sems, whole
        self.index, self.size = {}, {}
        self.sent = [0, 0]

    def group(self, key, size):
        self.index.setdefault(key, len(self.index))
        self.size[key] = self.size.get(key, 0) + size

    def send(self, key, src, dst, device, phase):
        pltpu.make_async_remote_copy(
            src_ref=src,
            dst_ref=dst,
            send_sem=self.send_sems.at[phase],
            recv_sem=self.recv_sems.at[self.index[key]],
            device_id=device,
            device_id_type=MESH,
        ).start()

    def wait(self, key):
        part = self.whole.at[pl.ds(0, self.size[key])]
        pltpu.make_async_copy(part, part, self.recv_sems.at[self.index[key]]).wait()

    def drain(self, phase):
        part = self.whole.at[pl.ds(0, self.sent[phase])]
        pltpu.make_async_copy(part, part, self.send_sems.at[phase]).wait()


class Sum:
    def __init__(self, at, exchange, diff, recv, total):
        self.at, self.exchange = at, exchange
        self.diff, self.recv, self.total = diff, recv, total
        self.events, self.settled, self.taken = [], [], 0

    def copy_of(self, key, size, offsets):
        return (key, size * COLUMNS * 4, offsets)

    def expect(self, key, size, phase):
        self.exchange.group(key, size)
        self.exchange.sent[phase] += size

    def slot(self, size):
        self.taken += size
        return self.taken - size

    def add_into(self, start, size, places):
        value = self.diff[rows(start, size)]
        for place in places:
            value = value + self.recv[pl.ds(place, size)]
        self.diff[rows(start, size)] = value

    def scatter(self, key, src, place, size, offsets):
        src_ref, dst_ref = self.diff.at[rows(src, size)], self.recv.at[pl.ds(place, size)]
        self.exchange.send(key, src_ref, dst_ref, moved(self.at, offsets), 0)

    def gather(self, key, start, size, offsets):
        ref = self.total.at[rows(start, size)]
        self.exchange.send(key, ref, ref, moved(self.at, offsets), 1)

    def piece(self, axes, offsets):
        index = 0
        for axis in axes:
            by = dict(offsets).get(axis, 0)
            index = index * LENGTH[axis] + lax.rem(self.at[axis] + by, LENGTH[axis])
        return index

    def chunk(self, tag, levels, base, size, early, times, prepare, square, finish):
        self.early = early
        starts, sizes, kinds = [base], [size], []
        for level in levels:
            kind, axes = level.split(":")
            kinds.append((kind, axes))
            sizes.append(sizes[-1] // math.prod(LENGTH[a] for a in axes))
            starts.append(starts[-1] + self.piece(axes, ()) * sizes[-1])
        waits, cost, times = [], 0.15, dict(times)
        for i, (kind, axes) in enumerate(kinds):
            args = (tag, i, axes, starts[i], sizes[i + 1], starts[i + 1])
            reduce = self.reduce_ring if kind == "r" else self.reduce_direct
            waits, prepare = reduce(args, waits, prepare, cost, times.get(i, 0.0))
            cost = 0.05

        def settle(add=prepare):
            add()
            square(starts[-1], sizes[-1])

        self.settled.append(("settled", tag))
        prepare, gives, stream = settle, ("settled", tag), []
        for i in reversed(range(len(kinds))):
            kind, axes = kinds[i]
            if i == 0 and stream:
                waits, prepare = self.gather_stream(tag, waits, prepare, stream, sizes[1])
                continue
            args = (tag, i, axes, starts[i], sizes[i + 1], starts[i + 1])
            onward = i == 1 and kinds[0][1] == "x" and kind == "r"
            build = self.gather_ring if kind == "r" else self.gather_direct
            begun = len(self.events)
            waits, prepare, stream = build(args, waits, prepare, gives, onward)
            self.events[begun].start = times.get(-1 - i, 0.0)
            gives = None
        self.events.append(Event(waits, prepare, gives=("end", tag)))
        self.events.append(Event([("end", tag), "factor"], lambda: finish(base, size), cost=0.2))

    def reduce_direct(self, args, waits, prepare, cost, start_time):
        tag, i, axes, start, part, mine = args
        key, offsets = (tag, "rs", i), others(axes)
        places = [self.slot(part) for _ in offsets]
        for _ in offsets:
            self.expect(key, part, 0)

        def run():
            prepare()
            for o, place in zip(offsets, places):
                self.scatter(key, start + self.piece(axes, o) * part, place, part, o)

        sends = [self.copy_of(key, part, o) for o in offsets]
        self.events.append(Event(waits, run, sends, cost, start=start_time))

        def after():
            self.exchange.wait(key)
            self.add_into(mine, part, places)

        return [key], after

    def reduce_ring(self, args, waits, prepare, cost, start_time):
        tag, i, axis, start, part, mine = args
        half, early = part // 2, self.early
        far = (tag, "far", i)
        near = (tag, "near", i)
        far_at = {1: self.slot(half), 3: self.slot(half)}
        near_at = {(by, h): self.slot(half) for by in (1, 3) for h in (0, 1)}
        for by in (1, 3):
            self.expect(far, half, 0)
            self.expect(near, part, 0)

        def quarter(by, h):
            return start + lax.rem(self.at[axis] + by, 4) * part + h * half

        def run():
            prepare()
            for by, h in ((1, 0), (3, 1)):
                self.scatter(far, quarter(2, h), far_at[by], half, ((axis, by),))
            if early:
                for by, h in ((1, 1), (3, 0)):
                    self.scatter(near, quarter(by, h), near_at[by, h], half, ((axis, by),))

        sends = [self.copy_of(far, half, ((axis, by),)) for by in (1, 3)]
        sends += [self.copy_of(near, half, ((axis, by),)) for by in (1, 3)] * early
        self.events.append(Event(waits, run, sends, cost, start=start_time))

        def pass_on():
            self.exchange.wait(far)
            for by, h in ((1, 0), (3, 1)):
                self.add_into(quarter(by, h), half, [far_at[by]])
            for by, h in ((1, 0), (3, 1)) if early else ((1, 0), (3, 1), (1, 1), (3, 0)):
                self.scatter(near, quarter(by, h), near_at[by, h], half, ((axis, by),))

        sends = [self.copy_of(near, half, ((axis, by),)) for by in (1, 3)]
        self.events.append(Event([far], pass_on, sends * (1 if early else 2), 0.06))

        def after():
            self.exchange.wait(near)
            for h in (0, 1):
                self.add_into(mine + h * half, half, [near_at[1, h], near_at[3, h]])

        return [near], after

    def gather_direct(self, args, waits, prepare, gives, onward):
        tag, i, axes, _, part, mine = args
        key, offsets = (tag, "ag", i), others(axes)
        for _ in offsets:
            self.expect(key, part, 1)

        def run():
            prepare()
            for o in offsets:
                self.gather(key, mine, part, o)

        self.events.append(Event(waits, run, [self.copy_of(key, part, o) for o in offsets], 0.05, gives))
        return [key], lambda: self.exchange.wait(key), None

    def gather_ring(self, args, waits, prepare, gives, onward):
        tag, i, axis, start, part, mine = args
        half = part // 2
        on = (tag, "on", i)
        end, cross = (tag, "end", i), (tag, "cross")
        across = (("x", 1),)
        for by in (1, 3):
            self.expect(on, half, 1)
            self.expect(end, part, 1)
        if onward:
            self.expect(cross, 4 * part, 1)

        def quarter(by, h):
            return start + lax.rem(self.at[axis] + by, 4) * part + h * half

        def run():
            prepare()
            for by, h in ((1, 0), (3, 1)):
                self.gather(on, mine + h * half, half, ((axis, by),))
            for by, h in ((1, 1), (3, 0)):
                self.gather(end, mine + h * half, half, ((axis, by),))
            if onward:
                self.gather(cross, mine, part, across)

        sends = [self.copy_of(on, half, ((axis, by),)) for by in (1, 3)]
        sends += [self.copy_of(end, half, ((axis, by),)) for by in (1, 3)]
        sends += [self.copy_of(cross, part, across)] * onward
        self.events.append(Event(waits, run, sends, 0.05, gives))

        def pass_on():
            self.exchange.wait(on)
            for by, h in ((1, 0), (3, 1)):
                self.gather(end, quarter(4 - by, h), half, ((axis, by),))
            if onward:
                for by, h in ((1, 0), (3, 1)):
                    self.gather(cross, quarter(4 - by, h), half, across)

        sends = [self.copy_of(end, half, ((axis, by),)) for by in (1, 3)]
        sends += [self.copy_of(cross, half, across)] * (2 * onward)
        self.events.append(Event([on], pass_on, sends, 0.03))

        def after():
            self.exchange.wait(end)

        def stream():
            self.gather(cross, quarter(3, 1), half, across)
            self.gather(cross, quarter(1, 0), half, across)
            self.gather(cross, quarter(2, 0), part, across)

        return [end], after, (stream, [half, half, part]) if onward else None

    def gather_stream(self, tag, waits, prepare, stream, size):
        stream, parts = stream
        key = (tag, "cross")

        def run():
            prepare()
            stream()

        self.events.append(Event(waits, run, [self.copy_of(key, n, (("x", 1),)) for n in parts], 0.05))
        return [key], lambda: self.exchange.wait(key)


def norm_events(at, settled, squares, parts, recv_sems, send_sem, finish):
    events, base, friends = [], 0, []
    mp = lax.axis_index("mp")
    rounds = [[(moved(at, o), o) for o in others("yz")]]
    last = []
    for flip in (0, 1):
        for by in range(4):
            if flip or by:
                o = (("x", 1),)
                last.append((dict(moved(at, o if flip else ()), mp=lax.rem(mp + by, 4)), o))
    rounds.append(last)
    waits = settled
    for i, peers in enumerate(rounds):
        key, part = ("norm", i), pl.ds(base, len(peers))

        def run(i=i, peers=peers, base=base):
            if i:
                add(i - 1)
            for j, (device, _) in enumerate(peers):
                pltpu.make_async_remote_copy(
                    src_ref=squares.at[i],
                    dst_ref=parts.at[base + j],
                    send_sem=send_sem,
                    recv_sem=recv_sems.at[i],
                    device_id=device,
                    device_id_type=MESH,
                ).start()

        events.append(Event(waits, run, [(key, 4096, o) for _, o in peers], 0.05))
        waits, base = [key], base + len(peers)
        friends += [device for device, _ in peers]

    def add(i):
        start = sum(len(p) for p in rounds[:i])
        n = len(rounds[i])
        part = parts.at[pl.ds(start, n)]
        pltpu.make_async_copy(part, part, recv_sems.at[i]).wait()
        value = squares[i]
        for j in range(n):
            value = value + parts[start + j]
        squares[i + 1] = value

    def end():
        add(1)
        finish()

    events.append(Event(waits, end, cost=0.2, gives="factor"))

    def drain():
        pltpu.make_async_copy(parts, parts, send_sem).wait()

    return events, friends, drain


def kernel(
    max_norm, count, slow, fast, momentum, slow_out, momentum_out, fast_out,
    slow_in, fast_in, momentum_in, diff, recv, total, squares, parts, factor,
    load_sems, recv_sems, send_sems, norm_sems, tokens,
):
    dp = lax.axis_index("dp")
    at = {"y": dp // 8, "z": lax.rem(dp // 2, 4), "x": lax.rem(dp, 2)}
    loads, base = [], 0
    for i, size in enumerate(LOADS):
        part = pl.ds(base, size)
        pair = []
        for j, (src, dst) in enumerate(((slow, slow_in), (fast, fast_in))):
            pair.append(pltpu.make_async_copy(src.at[part], dst.at[part], load_sems.at[2 * i + j]))
            pair[-1].start()
        loads.append((base + size, pair))
        base += size
    late = pltpu.make_async_copy(momentum, momentum_in, load_sems.at[2 * len(LOADS)])
    squares[0] = jnp.zeros(squares.shape[1:], squares.dtype)

    def load(base, size):
        def run():
            while loads and (not ready[0] or ready[0] < base + size):
                ready[0], pair = loads.pop(0)
                for copy in pair:
                    copy.wait()
            part = pl.ds(base, size)
            diff[part] = slow_in[part] - fast_in[part].astype(jnp.float32)

        return run

    ready = [0]

    def square(start, size):
        value = diff[rows(start, size)]
        total[rows(start, size)] = value
        value = value * value
        value = value[:, :128] + value[:, 128:]
        squares[0] += value.reshape(size // 8, 8, 128).sum(axis=0)

    def clip():
        norm = jnp.sqrt(jnp.sum(squares[2], axis=(0, 1), keepdims=True)) / count
        scale = jnp.minimum(1.0, max_norm / (norm + EPSILON)) / count
        factor[...] = jnp.broadcast_to(scale, factor.shape)
        late.wait()

    def finish(base, size):
        part = pl.ds(base, size)
        scale = jnp.concatenate([factor[0:1], factor[0:1]], axis=1)
        gradient = scale * total[part]
        momentum_next = MOMENTUM_RATE * momentum_in[part] + gradient
        slow_next = slow_in[part] - OUTER_RATE * (gradient + MOMENTUM_RATE * momentum_next)
        momentum_out[part] = momentum_next
        slow_out[part] = slow_next
        fast_out[part] = slow_next.astype(fast_out.dtype)

    exchange = Exchange(recv_sems, send_sems, total)
    work = Sum(at, exchange, diff, recv, total)
    base = 0
    for tag, (levels, size, early, times) in enumerate(CHUNKS):
        work.chunk(tag, levels, base, size, early, times, load(base, size), square, finish)
        base += size
    events, friends, drain = norm_events(
        at, work.settled, squares, parts, norm_sems, send_sems.at[2], clip
    )
    events, _ = in_order(work.events + events)

    near = [moved(at, ((axis, by),)) for axis in "yz" for by in (1, 3)]
    partner = moved(at, (("x", 1),))
    barrier = pltpu.get_barrier_semaphore()
    for device in near + friends[-7:]:
        pl.semaphore_signal(barrier, inc=1, device_id=device, device_id_type=MESH)
    pl.semaphore_wait(barrier, len(near) + 7)

    def tell(i):
        for device in near + [partner]:
            pl.semaphore_signal(tokens.at[i], inc=1, device_id=device, device_id_type=MESH)

    def hear(i):
        pl.semaphore_wait(tokens.at[i], len(near) + 1)

    tell(0)
    distant = [any(steps(hops) > 1 for _, _, hops in event.sends) for event in events].index(True)
    for i, event in enumerate(events):
        if i == len(CHUNKS):
            late.start()
        if i == min(len(CHUNKS) + 2, distant):
            hear(0)
            tell(1)
        if i == distant:
            hear(1)
        event.run()
    exchange.drain(0)
    exchange.drain(1)
    drain()


def updated(slow, fast, momentum, max_norm, count):
    f32, shape = jnp.float32, slow.shape
    hbm = pl.BlockSpec(memory_space=pltpu.HBM)
    vmem = pl.BlockSpec(memory_space=pltpu.VMEM)
    groups = sum(2 if level[0] == "d" else 4 for chunk in CHUNKS for level in chunk[0])
    return pl.pallas_call(
        lambda *refs: kernel(max_norm, count, *refs),
        out_shape=(pltpu.VMEM(shape, f32), pltpu.VMEM(shape, f32), pltpu.VMEM(shape, fast.dtype)),
        in_specs=[hbm, hbm, hbm],
        out_specs=(vmem, vmem, vmem),
        scratch_shapes=[
            pltpu.VMEM(shape, f32),
            pltpu.VMEM(shape, fast.dtype),
            pltpu.VMEM(shape, f32),
            pltpu.VMEM(shape, f32),
            pltpu.VMEM(shape, f32),
            pltpu.VMEM(shape, f32),
            pltpu.VMEM((3, 8, 128), f32),
            pltpu.VMEM((22, 8, 128), f32),
            pltpu.VMEM((8, 128), f32),
            pltpu.SemaphoreType.DMA((2 * len(LOADS) + 1,)),
            pltpu.SemaphoreType.DMA((groups,)),
            pltpu.SemaphoreType.DMA((3,)),
            pltpu.SemaphoreType.DMA((2,)),
            pltpu.SemaphoreType.REGULAR((2,)),
        ],
        compiler_params=pltpu.CompilerParams(
            collective_id=0, has_side_effects=True, vmem_limit_bytes=40 * 1024 * 1024
        ),
        name="updated",
    )(*(pltpu.with_memory_space_constraint(x, pltpu.HBM) for x in (slow, fast, momentum)))


def written(*values):
    def run(*refs):
        n = len(values)
        copies = [pltpu.make_async_copy(refs[i], refs[n + i], refs[-1].at[i]) for i in range(n)]
        for copy in copies:
            copy.start()
        for copy in copies:
            copy.wait()

    return pl.pallas_call(
        run,
        out_shape=tuple(pltpu.HBM(x.shape, x.dtype) for x in values),
        in_specs=[pl.BlockSpec(memory_space=pltpu.VMEM)] * len(values),
        out_specs=tuple(pl.BlockSpec(memory_space=pltpu.HBM) for _ in values),
        scratch_shapes=[pltpu.SemaphoreType.DMA((len(values),))],
        compiler_params=pltpu.CompilerParams(vmem_limit_bytes=1024 * 1024),
        name="written",
    )(*(pltpu.with_memory_space_constraint(x, pltpu.VMEM) for x in values))


def body(slow_weights, fast_weights, momentum):
    replicas = lax.axis_size("dp")
    entries = slow_weights.shape[0] * slow_weights.shape[1] * slow_weights.shape[2] * lax.axis_size("mp")
    max_norm = CLIP_LEVEL * math.sqrt(entries)
    values = updated(slow_weights[0], fast_weights[0, 0], momentum[0], max_norm, replicas)
    slow_next, momentum_next, fast_next = written(*values)
    return (slow_next[None], momentum_next[None], fast_next[None, None])


def solution(mesh):
    in_specs = (P(None, None, "mp"), P("dp", None, None, "mp"), P(None, None, "mp"))
    out_specs = (P(None, None, "mp"), P(None, None, "mp"), P("dp", None, None, "mp"))
    return jax.shard_map(body, mesh=mesh, in_specs=in_specs, out_specs=out_specs, check_vma=False)
```

```python
import math

import jax
import jax.numpy as jnp
from jax import lax
from jax.experimental import pallas as pl
from jax.experimental.pallas import tpu as pltpu
from jax.sharding import PartitionSpec as P

MOMENTUM_RATE = 0.9
OUTER_RATE = 0.7
CLIP_LEVEL = 0.2
EPSILON = 1e-06

MESH = pl.DeviceIdType.MESH
LENGTH = {"x": 2, "y": 4, "z": 4}
COLUMNS = 256
Y, Z = ("r:y", "d:zx"), ("r:z", "d:yx")
YX, ZX = ("r:y", "d:x", "d:z"), ("r:z", "d:x", "d:y")
XY, XZ = ("d:x", "d:y", "d:z"), ("d:x", "d:z", "d:y")
CHUNKS = (
    (Z, 256, True, ((-2, 6.0), (-1, 20.8),)),
    (Z, 256, False, ((-3, 18.1), (-2, 13.7), (-1, 17.1), (0, 5.3),)),
    (YX, 256, False, ((-1, 15.9),)),
    (XY, 256, False, ((-2, 8.0), (1, 6.3),)),
    (Z, 256, True, ((-1, 0), (0, 5.9),)),
    (YX, 256, True, ((-3, 10.1), (-2, 10.1), (-1, 17.2),)),
    (YX, 256, True, ((-1, 9.3), (1, 0),)),
    (Z, 256, False, ((-2, 0), (-1, 20.7), (0, 7.7), (1, 14.2),)),
    (Z, 256, True, ((-3, 8.6), (-1, 2.6),)),
    (XY, 256, True, ((-3, 17.7), (-2, 23.0), (-1, 19.6), (1, 5.9),)),
    (XY, 256, False, ((-3, 1.0), (-1, 6.8),)),
    (YX, 256, False, ((-2, 6.4), (-1, 19.2),)),
    (Z, 256, True, ((-1, 7.8), (0, 0),)),
    (Z, 256, False, ((-3, 3.0), (1, 10.7),)),
)
LOADS = (512, 768, 1024, 1280)
RATE = 45e3
HOP = (2.7, 0.5)
ISSUE = 0.01
COST = 0.4


class Event:
    def __init__(self, waits, run, sends=(), cost=0.02, gives=None, start=0.0):
        self.waits, self.run, self.sends = waits, run, sends
        self.cost, self.gives, self.start = cost, gives, start


def in_order(events):
    arrival, free, now, left, done = {}, {}, 0.0, list(events), []
    need = {}
    for event in events:
        for key, _, _ in event.sends:
            need[key] = need.get(key, 0) + 1
    while left:
        best = None
        for event in left:
            if all(w in arrival and not need.get(w) for w in event.waits):
                ready = max([event.start] + [arrival[w] for w in event.waits])
                if best is None or max(ready, now) < max(best[0], now):
                    best = (ready, event)
        ready, event = best
        left.remove(event)
        done.append(event)
        now = max(now, ready) + COST * event.cost
        for key, size, hops in event.sends:
            now += ISSUE
            end = now
            for axis, by in hops:
                ways = {"y": {1: "+", 3: "-", 2: "+-"}, "z": {1: "+", 3: "-", 2: "+-"}, "x": {1: "+-"}}[axis][by]
                for way in ways:
                    begin = max(now, free.get(axis + way, 0.0))
                    free[axis + way] = begin + size / RATE
                    end = max(end, begin + size / RATE)
            count = sum(2 if axis == "x" else min(by, 4 - by) for axis, by in hops)
            arrival[key] = max(arrival.get(key, 0.0), end + HOP[0] + HOP[1] * count)
            need[key] -= 1
        if event.gives is not None:
            arrival[event.gives] = now
    return done, now


def moved(at, offsets):
    to = dict(at)
    for axis, by in offsets:
        to[axis] = lax.rem(at[axis] + by, LENGTH[axis])
    return {"dp": (to["y"] * 4 + to["z"]) * 2 + to["x"]}


def others(axes):
    found = [()]
    for axis in axes:
        found = [o + ((axis, by),) for o in found for by in range(LENGTH[axis])]
    return [tuple((a, by) for a, by in o if by) for o in found if any(by for _, by in o)]


def steps(offsets):
    return sum(min(by, LENGTH[axis] - by) for axis, by in offsets)


def rows(start, size):
    return pl.ds(start if isinstance(start, int) else pl.multiple_of(start, 8), size)


class Exchange:
    def __init__(self, recv_sems, send_sems, whole):
        self.recv_sems, self.send_sems, self.whole = recv_sems, send_sems, whole
        self.index, self.size = {}, {}
        self.sent = [0, 0]

    def group(self, key, size):
        self.index.setdefault(key, len(self.index))
        self.size[key] = self.size.get(key, 0) + size

    def send(self, key, src, dst, device, phase):
        pltpu.make_async_remote_copy(
            src_ref=src,
            dst_ref=dst,
            send_sem=self.send_sems.at[phase],
            recv_sem=self.recv_sems.at[self.index[key]],
            device_id=device,
            device_id_type=MESH,
        ).start()

    def wait(self, key):
        part = self.whole.at[pl.ds(0, self.size[key])]
        pltpu.make_async_copy(part, part, self.recv_sems.at[self.index[key]]).wait()

    def drain(self, phase):
        part = self.whole.at[pl.ds(0, self.sent[phase])]
        pltpu.make_async_copy(part, part, self.send_sems.at[phase]).wait()


class Sum:
    def __init__(self, at, exchange, diff, recv, total):
        self.at, self.exchange = at, exchange
        self.diff, self.recv, self.total = diff, recv, total
        self.events, self.settled, self.taken = [], [], 0

    def copy_of(self, key, size, offsets):
        return (key, size * COLUMNS * 4, offsets)

    def expect(self, key, size, phase):
        self.exchange.group(key, size)
        self.exchange.sent[phase] += size

    def slot(self, size):
        self.taken += size
        return self.taken - size

    def add_into(self, start, size, places):
        value = self.diff[rows(start, size)]
        for place in places:
            value = value + self.recv[pl.ds(place, size)]
        self.diff[rows(start, size)] = value

    def scatter(self, key, src, place, size, offsets):
        src_ref, dst_ref = self.diff.at[rows(src, size)], self.recv.at[pl.ds(place, size)]
        self.exchange.send(key, src_ref, dst_ref, moved(self.at, offsets), 0)

    def gather(self, key, start, size, offsets):
        ref = self.total.at[rows(start, size)]
        self.exchange.send(key, ref, ref, moved(self.at, offsets), 1)

    def piece(self, axes, offsets):
        index = 0
        for axis in axes:
            by = dict(offsets).get(axis, 0)
            index = index * LENGTH[axis] + lax.rem(self.at[axis] + by, LENGTH[axis])
        return index

    def chunk(self, tag, levels, base, size, early, times, prepare, square, finish):
        self.early = early
        starts, sizes, kinds = [base], [size], []
        for level in levels:
            kind, axes = level.split(":")
            kinds.append((kind, axes))
            sizes.append(sizes[-1] // math.prod(LENGTH[a] for a in axes))
            starts.append(starts[-1] + self.piece(axes, ()) * sizes[-1])
        waits, cost, times = [], 0.15, dict(times)
        for i, (kind, axes) in enumerate(kinds):
            args = (tag, i, axes, starts[i], sizes[i + 1], starts[i + 1])
            reduce = self.reduce_ring if kind == "r" else self.reduce_direct
            waits, prepare = reduce(args, waits, prepare, cost, times.get(i, 0.0))
            cost = 0.05

        def settle(add=prepare):
            add()
            square(starts[-1], sizes[-1])

        self.settled.append(("settled", tag))
        prepare, gives, stream = settle, ("settled", tag), []
        for i in reversed(range(len(kinds))):
            kind, axes = kinds[i]
            if i == 0 and stream:
                waits, prepare = self.gather_stream(tag, waits, prepare, stream, sizes[1])
                continue
            args = (tag, i, axes, starts[i], sizes[i + 1], starts[i + 1])
            onward = i == 1 and kinds[0][1] == "x" and kind == "r"
            build = self.gather_ring if kind == "r" else self.gather_direct
            begun = len(self.events)
            waits, prepare, stream = build(args, waits, prepare, gives, onward)
            self.events[begun].start = times.get(-1 - i, 0.0)
            gives = None
        self.events.append(Event(waits, prepare, gives=("end", tag)))
        self.events.append(Event([("end", tag), "factor"], lambda: finish(base, size), cost=0.2))

    def reduce_direct(self, args, waits, prepare, cost, start_time):
        tag, i, axes, start, part, mine = args
        key, offsets = (tag, "rs", i), others(axes)
        places = [self.slot(part) for _ in offsets]
        for _ in offsets:
            self.expect(key, part, 0)

        def run():
            prepare()
            for o, place in zip(offsets, places):
                self.scatter(key, start + self.piece(axes, o) * part, place, part, o)

        sends = [self.copy_of(key, part, o) for o in offsets]
        self.events.append(Event(waits, run, sends, cost, start=start_time))

        def after():
            self.exchange.wait(key)
            self.add_into(mine, part, places)

        return [key], after

    def reduce_ring(self, args, waits, prepare, cost, start_time):
        tag, i, axis, start, part, mine = args
        half, early = part // 2, self.early
        far = (tag, "far", i)
        near = (tag, "near", i)
        far_at = {1: self.slot(half), 3: self.slot(half)}
        near_at = {(by, h): self.slot(half) for by in (1, 3) for h in (0, 1)}
        for by in (1, 3):
            self.expect(far, half, 0)
            self.expect(near, part, 0)

        def quarter(by, h):
            return start + lax.rem(self.at[axis] + by, 4) * part + h * half

        def run():
            prepare()
            for by, h in ((1, 0), (3, 1)):
                self.scatter(far, quarter(2, h), far_at[by], half, ((axis, by),))
            if early:
                for by, h in ((1, 1), (3, 0)):
                    self.scatter(near, quarter(by, h), near_at[by, h], half, ((axis, by),))

        sends = [self.copy_of(far, half, ((axis, by),)) for by in (1, 3)]
        sends += [self.copy_of(near, half, ((axis, by),)) for by in (1, 3)] * early
        self.events.append(Event(waits, run, sends, cost, start=start_time))

        def pass_on():
            self.exchange.wait(far)
            for by, h in ((1, 0), (3, 1)):
                self.add_into(quarter(by, h), half, [far_at[by]])
            for by, h in ((1, 0), (3, 1)) if early else ((1, 0), (3, 1), (1, 1), (3, 0)):
                self.scatter(near, quarter(by, h), near_at[by, h], half, ((axis, by),))

        sends = [self.copy_of(near, half, ((axis, by),)) for by in (1, 3)]
        self.events.append(Event([far], pass_on, sends * (1 if early else 2), 0.06))

        def after():
            self.exchange.wait(near)
            for h in (0, 1):
                self.add_into(mine + h * half, half, [near_at[1, h], near_at[3, h]])

        return [near], after

    def gather_direct(self, args, waits, prepare, gives, onward):
        tag, i, axes, _, part, mine = args
        key, offsets = (tag, "ag", i), others(axes)
        for _ in offsets:
            self.expect(key, part, 1)

        def run():
            prepare()
            for o in offsets:
                self.gather(key, mine, part, o)

        self.events.append(Event(waits, run, [self.copy_of(key, part, o) for o in offsets], 0.05, gives))
        return [key], lambda: self.exchange.wait(key), None

    def gather_ring(self, args, waits, prepare, gives, onward):
        tag, i, axis, start, part, mine = args
        half = part // 2
        on = (tag, "on", i)
        end, cross = (tag, "end", i), (tag, "cross")
        across = (("x", 1),)
        for by in (1, 3):
            self.expect(on, half, 1)
            self.expect(end, part, 1)
        if onward:
            self.expect(cross, 4 * part, 1)

        def quarter(by, h):
            return start + lax.rem(self.at[axis] + by, 4) * part + h * half

        def run():
            prepare()
            for by, h in ((1, 0), (3, 1)):
                self.gather(on, mine + h * half, half, ((axis, by),))
            for by, h in ((1, 1), (3, 0)):
                self.gather(end, mine + h * half, half, ((axis, by),))
            if onward:
                self.gather(cross, mine, part, across)

        sends = [self.copy_of(on, half, ((axis, by),)) for by in (1, 3)]
        sends += [self.copy_of(end, half, ((axis, by),)) for by in (1, 3)]
        sends += [self.copy_of(cross, part, across)] * onward
        self.events.append(Event(waits, run, sends, 0.05, gives))

        def pass_on():
            self.exchange.wait(on)
            for by, h in ((1, 0), (3, 1)):
                self.gather(end, quarter(4 - by, h), half, ((axis, by),))
            if onward:
                for by, h in ((1, 0), (3, 1)):
                    self.gather(cross, quarter(4 - by, h), half, across)

        sends = [self.copy_of(end, half, ((axis, by),)) for by in (1, 3)]
        sends += [self.copy_of(cross, half, across)] * (2 * onward)
        self.events.append(Event([on], pass_on, sends, 0.03))

        def after():
            self.exchange.wait(end)

        def stream():
            self.gather(cross, quarter(3, 1), half, across)
            self.gather(cross, quarter(1, 0), half, across)
            self.gather(cross, quarter(2, 0), part, across)

        return [end], after, (stream, [half, half, part]) if onward else None

    def gather_stream(self, tag, waits, prepare, stream, size):
        stream, parts = stream
        key = (tag, "cross")

        def run():
            prepare()
            stream()

        self.events.append(Event(waits, run, [self.copy_of(key, n, (("x", 1),)) for n in parts], 0.05))
        return [key], lambda: self.exchange.wait(key)


def norm_events(at, settled, squares, parts, recv_sems, send_sem, finish):
    events, base, friends = [], 0, []
    mp = lax.axis_index("mp")
    rounds = [[(moved(at, o), o) for o in others("yz")]]
    last = []
    for flip in (0, 1):
        for by in range(4):
            if flip or by:
                o = (("x", 1),)
                last.append((dict(moved(at, o if flip else ()), mp=lax.rem(mp + by, 4)), o))
    rounds.append(last)
    waits = settled
    for i, peers in enumerate(rounds):
        key, part = ("norm", i), pl.ds(base, len(peers))

        def run(i=i, peers=peers, base=base):
            if i:
                add(i - 1)
            for j, (device, _) in enumerate(peers):
                pltpu.make_async_remote_copy(
                    src_ref=squares.at[i],
                    dst_ref=parts.at[base + j],
                    send_sem=send_sem,
                    recv_sem=recv_sems.at[i],
                    device_id=device,
                    device_id_type=MESH,
                ).start()

        events.append(Event(waits, run, [(key, 4096, o) for _, o in peers], 0.05))
        waits, base = [key], base + len(peers)
        friends += [device for device, _ in peers]

    def add(i):
        start = sum(len(p) for p in rounds[:i])
        n = len(rounds[i])
        part = parts.at[pl.ds(start, n)]
        pltpu.make_async_copy(part, part, recv_sems.at[i]).wait()
        value = squares[i]
        for j in range(n):
            value = value + parts[start + j]
        squares[i + 1] = value

    def end():
        add(1)
        finish()

    events.append(Event(waits, end, cost=0.2, gives="factor"))

    def drain():
        pltpu.make_async_copy(parts, parts, send_sem).wait()

    return events, friends, drain


def kernel(
    max_norm, count, slow, fast, momentum, slow_out, momentum_out, fast_out,
    slow_in, fast_in, momentum_in, diff, recv, total, squares, parts, factor,
    load_sems, recv_sems, send_sems, norm_sems, tokens,
):
    dp = lax.axis_index("dp")
    at = {"y": dp // 8, "z": lax.rem(dp // 2, 4), "x": lax.rem(dp, 2)}
    loads, base = [], 0
    for i, size in enumerate(LOADS):
        part = pl.ds(base, size)
        pair = []
        for j, (src, dst) in enumerate(((slow, slow_in), (fast, fast_in))):
            pair.append(pltpu.make_async_copy(src.at[part], dst.at[part], load_sems.at[2 * i + j]))
            pair[-1].start()
        loads.append((base + size, pair))
        base += size
    late = pltpu.make_async_copy(momentum, momentum_in, load_sems.at[2 * len(LOADS)])
    squares[0] = jnp.zeros(squares.shape[1:], squares.dtype)

    def load(base, size):
        def run():
            while loads and (not ready[0] or ready[0] < base + size):
                ready[0], pair = loads.pop(0)
                for copy in pair:
                    copy.wait()
            part = pl.ds(base, size)
            diff[part] = slow_in[part] - fast_in[part].astype(jnp.float32)

        return run

    ready = [0]

    def square(start, size):
        value = diff[rows(start, size)]
        total[rows(start, size)] = value
        value = value * value
        value = value[:, :128] + value[:, 128:]
        squares[0] += value.reshape(size // 8, 8, 128).sum(axis=0)

    def clip():
        norm = jnp.sqrt(jnp.sum(squares[2], axis=(0, 1), keepdims=True)) / count
        scale = jnp.minimum(1.0, max_norm / (norm + EPSILON)) / count
        factor[...] = jnp.broadcast_to(scale, factor.shape)
        late.wait()

    def finish(base, size):
        part = pl.ds(base, size)
        scale = jnp.concatenate([factor[0:1], factor[0:1]], axis=1)
        gradient = scale * total[part]
        momentum_next = MOMENTUM_RATE * momentum_in[part] + gradient
        slow_next = slow_in[part] - OUTER_RATE * (gradient + MOMENTUM_RATE * momentum_next)
        momentum_out[part] = momentum_next
        slow_out[part] = slow_next
        fast_out[part] = slow_next.astype(fast_out.dtype)

    exchange = Exchange(recv_sems, send_sems, total)
    work = Sum(at, exchange, diff, recv, total)
    base = 0
    for tag, (levels, size, early, times) in enumerate(CHUNKS):
        work.chunk(tag, levels, base, size, early, times, load(base, size), square, finish)
        base += size
    events, friends, drain = norm_events(
        at, work.settled, squares, parts, norm_sems, send_sems.at[2], clip
    )
    events, _ = in_order(work.events + events)

    near = [moved(at, ((axis, by),)) for axis in "yz" for by in (1, 3)]
    partner = moved(at, (("x", 1),))
    barrier = pltpu.get_barrier_semaphore()
    for device in near + friends[-7:]:
        pl.semaphore_signal(barrier, inc=1, device_id=device, device_id_type=MESH)
    pl.semaphore_wait(barrier, len(near) + 7)

    def tell(i):
        for device in near + [partner]:
            pl.semaphore_signal(tokens.at[i], inc=1, device_id=device, device_id_type=MESH)

    def hear(i):
        pl.semaphore_wait(tokens.at[i], len(near) + 1)

    tell(0)
    distant = [any(steps(hops) > 1 for _, _, hops in event.sends) for event in events].index(True)
    for i, event in enumerate(events):
        if i == len(CHUNKS):
            late.start()
        if i == min(len(CHUNKS) + 2, distant):
            hear(0)
            tell(1)
        if i == distant:
            hear(1)
        event.run()
    exchange.drain(0)
    exchange.drain(1)
    drain()


def updated(slow, fast, momentum, max_norm, count):
    f32, shape = jnp.float32, slow.shape
    hbm = pl.BlockSpec(memory_space=pltpu.HBM)
    vmem = pl.BlockSpec(memory_space=pltpu.VMEM)
    groups = sum(2 if level[0] == "d" else 4 for chunk in CHUNKS for level in chunk[0])
    return pl.pallas_call(
        lambda *refs: kernel(max_norm, count, *refs),
        out_shape=(pltpu.VMEM(shape, f32), pltpu.VMEM(shape, f32), pltpu.VMEM(shape, fast.dtype)),
        in_specs=[hbm, hbm, hbm],
        out_specs=(vmem, vmem, vmem),
        scratch_shapes=[
            pltpu.VMEM(shape, f32),
            pltpu.VMEM(shape, fast.dtype),
            pltpu.VMEM(shape, f32),
            pltpu.VMEM(shape, f32),
            pltpu.VMEM(shape, f32),
            pltpu.VMEM(shape, f32),
            pltpu.VMEM((3, 8, 128), f32),
            pltpu.VMEM((22, 8, 128), f32),
            pltpu.VMEM((8, 128), f32),
            pltpu.SemaphoreType.DMA((2 * len(LOADS) + 1,)),
            pltpu.SemaphoreType.DMA((groups,)),
            pltpu.SemaphoreType.DMA((3,)),
            pltpu.SemaphoreType.DMA((2,)),
            pltpu.SemaphoreType.REGULAR((2,)),
        ],
        compiler_params=pltpu.CompilerParams(
            collective_id=0, has_side_effects=True, vmem_limit_bytes=40 * 1024 * 1024
        ),
        name="updated",
    )(*(pltpu.with_memory_space_constraint(x, pltpu.HBM) for x in (slow, fast, momentum)))


def written(*values):
    def run(*refs):
        n = len(values)
        copies = [pltpu.make_async_copy(refs[i], refs[n + i], refs[-1].at[i]) for i in range(n)]
        for copy in copies:
            copy.start()
        for copy in copies:
            copy.wait()

    return pl.pallas_call(
        run,
        out_shape=tuple(pltpu.HBM(x.shape, x.dtype) for x in values),
        in_specs=[pl.BlockSpec(memory_space=pltpu.VMEM)] * len(values),
        out_specs=tuple(pl.BlockSpec(memory_space=pltpu.HBM) for _ in values),
        scratch_shapes=[pltpu.SemaphoreType.DMA((len(values),))],
        compiler_params=pltpu.CompilerParams(vmem_limit_bytes=1024 * 1024),
        name="written",
    )(*(pltpu.with_memory_space_constraint(x, pltpu.VMEM) for x in values))


def body(slow_weights, fast_weights, momentum):
    replicas = lax.axis_size("dp")
    entries = slow_weights.shape[0] * slow_weights.shape[1] * slow_weights.shape[2] * lax.axis_size("mp")
    max_norm = CLIP_LEVEL * math.sqrt(entries)
    values = updated(slow_weights[0], fast_weights[0, 0], momentum[0], max_norm, replicas)
    slow_next, momentum_next, fast_next = written(*values)
    return (slow_next[None], momentum_next[None], fast_next[None, None])


def solution(mesh):
    in_specs = (P(None, None, "mp"), P("dp", None, None, "mp"), P(None, None, "mp"))
    out_specs = (P(None, None, "mp"), P(None, None, "mp"), P("dp", None, None, "mp"))
    return jax.shard_map(body, mesh=mesh, in_specs=in_specs, out_specs=out_specs, check_vma=False)
```

```python
import math

import jax
import jax.numpy as jnp
from jax import lax
from jax.experimental import pallas as pl
from jax.experimental.pallas import tpu as pltpu
from jax.sharding import PartitionSpec as P

MOMENTUM_RATE = 0.9
OUTER_RATE = 0.7
CLIP_LEVEL = 0.2
EPSILON = 1e-06

MESH = pl.DeviceIdType.MESH
LENGTH = {"x": 2, "y": 4, "z": 4}
COLUMNS = 256
Y, Z = ("r:y", "d:zx"), ("r:z", "d:yx")
YX, ZX = ("r:y", "d:x", "d:z"), ("r:z", "d:x", "d:y")
XY, XZ = ("d:x", "d:y", "d:z"), ("d:x", "d:z", "d:y")
CHUNKS = (
    (Z, 256, True, ((-2, 6.0), (-1, 20.8),)),
    (Z, 256, True, ((-1, 0), (0, 5.9),)),
    (YX, 256, False, ((-1, 15.9),)),
    (Z, 256, False, ((-2, 0), (-1, 20.7), (0, 7.7), (1, 14.2),)),
    (XY, 256, True, ((-3, 17.7), (-2, 23.0), (-1, 18.3), (1, 5.9),)),
    (YX, 256, True, ((-3, 10.1), (-2, 10.1), (-1, 17.2),)),
    (Z, 256, False, ((-3, 18.1), (-2, 13.7), (-1, 17.1), (0, 5.3),)),
    (YX, 256, True, ((-3, 22.2), (-1, 9.3), (1, 0),)),
    (Z, 256, True, ((-3, 8.6), (-1, 2.6),)),
    (XY, 256, False, ((-3, 0), (-2, 8.0), (1, 6.3),)),
    (XY, 256, False, ((-3, 1.0), (-1, 6.8),)),
    (YX, 256, False, ((-2, 6.4), (-1, 19.2),)),
    (Z, 256, True, ((-1, 7.8), (0, 0),)),
    (Z, 256, False, ((-3, 3.0), (1, 10.7),)),
)
LOADS = (512, 768, 1024, 1280)
RATE = 45e3
HOP = (2.7, 0.5)
ISSUE = 0.01
COST = 0.4


class Event:
    def __init__(self, waits, run, sends=(), cost=0.02, gives=None, start=0.0):
        self.waits, self.run, self.sends = waits, run, sends
        self.cost, self.gives, self.start = cost, gives, start


def in_order(events):
    arrival, free, now, left, done = {}, {}, 0.0, list(events), []
    need = {}
    for event in events:
        for key, _, _ in event.sends:
            need[key] = need.get(key, 0) + 1
    while left:
        best = None
        for event in left:
            if all(w in arrival and not need.get(w) for w in event.waits):
                ready = max([event.start] + [arrival[w] for w in event.waits])
                if best is None or max(ready, now) < max(best[0], now):
                    best = (ready, event)
        ready, event = best
        left.remove(event)
        done.append(event)
        now = max(now, ready) + COST * event.cost
        for key, size, hops in event.sends:
            now += ISSUE
            end = now
            for axis, by in hops:
                ways = {"y": {1: "+", 3: "-", 2: "+-"}, "z": {1: "+", 3: "-", 2: "+-"}, "x": {1: "+-"}}[axis][by]
                for way in ways:
                    begin = max(now, free.get(axis + way, 0.0))
                    free[axis + way] = begin + size / RATE
                    end = max(end, begin + size / RATE)
            count = sum(2 if axis == "x" else min(by, 4 - by) for axis, by in hops)
            arrival[key] = max(arrival.get(key, 0.0), end + HOP[0] + HOP[1] * count)
            need[key] -= 1
        if event.gives is not None:
            arrival[event.gives] = now
    return done, now


def moved(at, offsets):
    to = dict(at)
    for axis, by in offsets:
        to[axis] = lax.rem(at[axis] + by, LENGTH[axis])
    return {"dp": (to["y"] * 4 + to["z"]) * 2 + to["x"]}


def others(axes):
    found = [()]
    for axis in axes:
        found = [o + ((axis, by),) for o in found for by in range(LENGTH[axis])]
    return [tuple((a, by) for a, by in o if by) for o in found if any(by for _, by in o)]


def steps(offsets):
    return sum(min(by, LENGTH[axis] - by) for axis, by in offsets)


def rows(start, size):
    return pl.ds(start if isinstance(start, int) else pl.multiple_of(start, 8), size)


class Exchange:
    def __init__(self, recv_sems, send_sems, whole):
        self.recv_sems, self.send_sems, self.whole = recv_sems, send_sems, whole
        self.index, self.size = {}, {}
        self.sent = [0, 0]

    def group(self, key, size):
        self.index.setdefault(key, len(self.index))
        self.size[key] = self.size.get(key, 0) + size

    def send(self, key, src, dst, device, phase):
        pltpu.make_async_remote_copy(
            src_ref=src,
            dst_ref=dst,
            send_sem=self.send_sems.at[phase],
            recv_sem=self.recv_sems.at[self.index[key]],
            device_id=device,
            device_id_type=MESH,
        ).start()

    def wait(self, key):
        part = self.whole.at[pl.ds(0, self.size[key])]
        pltpu.make_async_copy(part, part, self.recv_sems.at[self.index[key]]).wait()

    def drain(self, phase):
        part = self.whole.at[pl.ds(0, self.sent[phase])]
        pltpu.make_async_copy(part, part, self.send_sems.at[phase]).wait()


class Sum:
    def __init__(self, at, exchange, diff, recv, total):
        self.at, self.exchange = at, exchange
        self.diff, self.recv, self.total = diff, recv, total
        self.events, self.settled, self.taken = [], [], 0

    def copy_of(self, key, size, offsets):
        return (key, size * COLUMNS * 4, offsets)

    def expect(self, key, size, phase):
        self.exchange.group(key, size)
        self.exchange.sent[phase] += size

    def slot(self, size):
        self.taken += size
        return self.taken - size

    def add_into(self, start, size, places):
        value = self.diff[rows(start, size)]
        for place in places:
            value = value + self.recv[pl.ds(place, size)]
        self.diff[rows(start, size)] = value

    def scatter(self, key, src, place, size, offsets):
        src_ref, dst_ref = self.diff.at[rows(src, size)], self.recv.at[pl.ds(place, size)]
        self.exchange.send(key, src_ref, dst_ref, moved(self.at, offsets), 0)

    def gather(self, key, start, size, offsets):
        ref = self.total.at[rows(start, size)]
        self.exchange.send(key, ref, ref, moved(self.at, offsets), 1)

    def piece(self, axes, offsets):
        index = 0
        for axis in axes:
            by = dict(offsets).get(axis, 0)
            index = index * LENGTH[axis] + lax.rem(self.at[axis] + by, LENGTH[axis])
        return index

    def chunk(self, tag, levels, base, size, early, times, prepare, square, finish):
        self.early = early
        starts, sizes, kinds = [base], [size], []
        for level in levels:
            kind, axes = level.split(":")
            kinds.append((kind, axes))
            sizes.append(sizes[-1] // math.prod(LENGTH[a] for a in axes))
            starts.append(starts[-1] + self.piece(axes, ()) * sizes[-1])
        waits, cost, times = [], 0.15, dict(times)
        for i, (kind, axes) in enumerate(kinds):
            args = (tag, i, axes, starts[i], sizes[i + 1], starts[i + 1])
            reduce = self.reduce_ring if kind == "r" else self.reduce_direct
            waits, prepare = reduce(args, waits, prepare, cost, times.get(i, 0.0))
            cost = 0.05

        def settle(add=prepare):
            add()
            square(starts[-1], sizes[-1])

        self.settled.append(("settled", tag))
        prepare, gives, stream = settle, ("settled", tag), []
        for i in reversed(range(len(kinds))):
            kind, axes = kinds[i]
            if i == 0 and stream:
                waits, prepare = self.gather_stream(tag, waits, prepare, stream, sizes[1])
                continue
            args = (tag, i, axes, starts[i], sizes[i + 1], starts[i + 1])
            onward = i == 1 and kinds[0][1] == "x" and kind == "r"
            build = self.gather_ring if kind == "r" else self.gather_direct
            begun = len(self.events)
            waits, prepare, stream = build(args, waits, prepare, gives, onward)
            self.events[begun].start = times.get(-1 - i, 0.0)
            gives = None
        self.events.append(Event(waits, prepare, gives=("end", tag)))
        self.events.append(Event([("end", tag), "factor"], lambda: finish(base, size), cost=0.2))

    def reduce_direct(self, args, waits, prepare, cost, start_time):
        tag, i, axes, start, part, mine = args
        key, offsets = (tag, "rs", i), others(axes)
        places = [self.slot(part) for _ in offsets]
        for _ in offsets:
            self.expect(key, part, 0)

        def run():
            prepare()
            for o, place in zip(offsets, places):
                self.scatter(key, start + self.piece(axes, o) * part, place, part, o)

        sends = [self.copy_of(key, part, o) for o in offsets]
        self.events.append(Event(waits, run, sends, cost, start=start_time))

        def after():
            self.exchange.wait(key)
            self.add_into(mine, part, places)

        return [key], after

    def reduce_ring(self, args, waits, prepare, cost, start_time):
        tag, i, axis, start, part, mine = args
        half, early = part // 2, self.early
        far = (tag, "far", i)
        near = (tag, "near", i)
        far_at = {1: self.slot(half), 3: self.slot(half)}
        near_at = {(by, h): self.slot(half) for by in (1, 3) for h in (0, 1)}
        for by in (1, 3):
            self.expect(far, half, 0)
            self.expect(near, part, 0)

        def quarter(by, h):
            return start + lax.rem(self.at[axis] + by, 4) * part + h * half

        def run():
            prepare()
            for by, h in ((1, 0), (3, 1)):
                self.scatter(far, quarter(2, h), far_at[by], half, ((axis, by),))
            if early:
                for by, h in ((1, 1), (3, 0)):
                    self.scatter(near, quarter(by, h), near_at[by, h], half, ((axis, by),))

        sends = [self.copy_of(far, half, ((axis, by),)) for by in (1, 3)]
        sends += [self.copy_of(near, half, ((axis, by),)) for by in (1, 3)] * early
        self.events.append(Event(waits, run, sends, cost, start=start_time))

        def pass_on():
            self.exchange.wait(far)
            for by, h in ((1, 0), (3, 1)):
                self.add_into(quarter(by, h), half, [far_at[by]])
            for by, h in ((1, 0), (3, 1)) if early else ((1, 0), (3, 1), (1, 1), (3, 0)):
                self.scatter(near, quarter(by, h), near_at[by, h], half, ((axis, by),))

        sends = [self.copy_of(near, half, ((axis, by),)) for by in (1, 3)]
        self.events.append(Event([far], pass_on, sends * (1 if early else 2), 0.06))

        def after():
            self.exchange.wait(near)
            for h in (0, 1):
                self.add_into(mine + h * half, half, [near_at[1, h], near_at[3, h]])

        return [near], after

    def gather_direct(self, args, waits, prepare, gives, onward):
        tag, i, axes, _, part, mine = args
        key, offsets = (tag, "ag", i), others(axes)
        for _ in offsets:
            self.expect(key, part, 1)

        def run():
            prepare()
            for o in offsets:
                self.gather(key, mine, part, o)

        self.events.append(Event(waits, run, [self.copy_of(key, part, o) for o in offsets], 0.05, gives))
        return [key], lambda: self.exchange.wait(key), None

    def gather_ring(self, args, waits, prepare, gives, onward):
        tag, i, axis, start, part, mine = args
        half = part // 2
        on = (tag, "on", i)
        end, cross = (tag, "end", i), (tag, "cross")
        across = (("x", 1),)
        for by in (1, 3):
            self.expect(on, half, 1)
            self.expect(end, part, 1)
        if onward:
            self.expect(cross, 4 * part, 1)

        def quarter(by, h):
            return start + lax.rem(self.at[axis] + by, 4) * part + h * half

        def run():
            prepare()
            for by, h in ((1, 0), (3, 1)):
                self.gather(on, mine + h * half, half, ((axis, by),))
            for by, h in ((1, 1), (3, 0)):
                self.gather(end, mine + h * half, half, ((axis, by),))
            if onward:
                self.gather(cross, mine, part, across)

        sends = [self.copy_of(on, half, ((axis, by),)) for by in (1, 3)]
        sends += [self.copy_of(end, half, ((axis, by),)) for by in (1, 3)]
        sends += [self.copy_of(cross, part, across)] * onward
        self.events.append(Event(waits, run, sends, 0.05, gives))

        def pass_on():
            self.exchange.wait(on)
            for by, h in ((1, 0), (3, 1)):
                self.gather(end, quarter(4 - by, h), half, ((axis, by),))
            if onward:
                for by, h in ((1, 0), (3, 1)):
                    self.gather(cross, quarter(4 - by, h), half, across)

        sends = [self.copy_of(end, half, ((axis, by),)) for by in (1, 3)]
        sends += [self.copy_of(cross, half, across)] * (2 * onward)
        self.events.append(Event([on], pass_on, sends, 0.03))

        def after():
            self.exchange.wait(end)

        def stream():
            self.gather(cross, quarter(3, 1), half, across)
            self.gather(cross, quarter(1, 0), half, across)
            self.gather(cross, quarter(2, 0), part, across)

        return [end], after, (stream, [half, half, part]) if onward else None

    def gather_stream(self, tag, waits, prepare, stream, size):
        stream, parts = stream
        key = (tag, "cross")

        def run():
            prepare()
            stream()

        self.events.append(Event(waits, run, [self.copy_of(key, n, (("x", 1),)) for n in parts], 0.05))
        return [key], lambda: self.exchange.wait(key)


def norm_events(at, settled, squares, parts, recv_sems, send_sem, finish):
    events, base, friends = [], 0, []
    mp = lax.axis_index("mp")
    rounds = [[(moved(at, o), o) for o in others("yz")]]
    last = []
    for flip in (0, 1):
        for by in range(4):
            if flip or by:
                o = (("x", 1),)
                last.append((dict(moved(at, o if flip else ()), mp=lax.rem(mp + by, 4)), o))
    rounds.append(last)
    waits = settled
    for i, peers in enumerate(rounds):
        key, part = ("norm", i), pl.ds(base, len(peers))

        def run(i=i, peers=peers, base=base):
            if i:
                add(i - 1)
            for j, (device, _) in enumerate(peers):
                pltpu.make_async_remote_copy(
                    src_ref=squares.at[i],
                    dst_ref=parts.at[base + j],
                    send_sem=send_sem,
                    recv_sem=recv_sems.at[i],
                    device_id=device,
                    device_id_type=MESH,
                ).start()

        events.append(Event(waits, run, [(key, 4096, o) for _, o in peers], 0.05))
        waits, base = [key], base + len(peers)
        friends += [device for device, _ in peers]

    def add(i):
        start = sum(len(p) for p in rounds[:i])
        n = len(rounds[i])
        part = parts.at[pl.ds(start, n)]
        pltpu.make_async_copy(part, part, recv_sems.at[i]).wait()
        value = squares[i]
        for j in range(n):
            value = value + parts[start + j]
        squares[i + 1] = value

    def end():
        add(1)
        finish()

    events.append(Event(waits, end, cost=0.2, gives="factor"))

    def drain():
        pltpu.make_async_copy(parts, parts, send_sem).wait()

    return events, friends, drain


def kernel(
    max_norm, count, slow, fast, momentum, slow_out, momentum_out, fast_out,
    slow_in, fast_in, momentum_in, diff, recv, total, squares, parts, factor,
    load_sems, recv_sems, send_sems, norm_sems, tokens,
):
    dp = lax.axis_index("dp")
    at = {"y": dp // 8, "z": lax.rem(dp // 2, 4), "x": lax.rem(dp, 2)}
    loads, base = [], 0
    for i, size in enumerate(LOADS):
        part = pl.ds(base, size)
        pair = []
        for j, (src, dst) in enumerate(((slow, slow_in), (fast, fast_in))):
            pair.append(pltpu.make_async_copy(src.at[part], dst.at[part], load_sems.at[2 * i + j]))
            pair[-1].start()
        loads.append((base + size, pair))
        base += size
    late = pltpu.make_async_copy(momentum, momentum_in, load_sems.at[2 * len(LOADS)])
    squares[0] = jnp.zeros(squares.shape[1:], squares.dtype)

    def load(base, size):
        def run():
            while loads and (not ready[0] or ready[0] < base + size):
                ready[0], pair = loads.pop(0)
                for copy in pair:
                    copy.wait()
            part = pl.ds(base, size)
            diff[part] = slow_in[part] - fast_in[part].astype(jnp.float32)

        return run

    ready = [0]

    def square(start, size):
        value = diff[rows(start, size)]
        total[rows(start, size)] = value
        value = value * value
        value = value[:, :128] + value[:, 128:]
        squares[0] += value.reshape(size // 8, 8, 128).sum(axis=0)

    def clip():
        norm = jnp.sqrt(jnp.sum(squares[2], axis=(0, 1), keepdims=True)) / count
        scale = jnp.minimum(1.0, max_norm / (norm + EPSILON)) / count
        factor[...] = jnp.broadcast_to(scale, factor.shape)
        late.wait()

    def finish(base, size):
        part = pl.ds(base, size)
        scale = jnp.concatenate([factor[0:1], factor[0:1]], axis=1)
        gradient = scale * total[part]
        momentum_next = MOMENTUM_RATE * momentum_in[part] + gradient
        slow_next = slow_in[part] - OUTER_RATE * (gradient + MOMENTUM_RATE * momentum_next)
        momentum_out[part] = momentum_next
        slow_out[part] = slow_next
        fast_out[part] = slow_next.astype(fast_out.dtype)

    exchange = Exchange(recv_sems, send_sems, total)
    work = Sum(at, exchange, diff, recv, total)
    base = 0
    for tag, (levels, size, early, times) in enumerate(CHUNKS):
        work.chunk(tag, levels, base, size, early, times, load(base, size), square, finish)
        base += size
    events, friends, drain = norm_events(
        at, work.settled, squares, parts, norm_sems, send_sems.at[2], clip
    )
    events, _ = in_order(work.events + events)

    near = [moved(at, ((axis, by),)) for axis in "yz" for by in (1, 3)]
    partner = moved(at, (("x", 1),))
    barrier = pltpu.get_barrier_semaphore()
    for device in near + friends[-7:]:
        pl.semaphore_signal(barrier, inc=1, device_id=device, device_id_type=MESH)
    pl.semaphore_wait(barrier, len(near) + 7)

    def tell(i):
        for device in near + [partner]:
            pl.semaphore_signal(tokens.at[i], inc=1, device_id=device, device_id_type=MESH)

    def hear(i):
        pl.semaphore_wait(tokens.at[i], len(near) + 1)

    tell(0)
    distant = [any(steps(hops) > 1 for _, _, hops in event.sends) for event in events].index(True)
    for i, event in enumerate(events):
        if i == len(CHUNKS):
            late.start()
        if i == min(len(CHUNKS) + 2, distant):
            hear(0)
            tell(1)
        if i == distant:
            hear(1)
        event.run()
    exchange.drain(0)
    exchange.drain(1)
    drain()


def updated(slow, fast, momentum, max_norm, count):
    f32, shape = jnp.float32, slow.shape
    hbm = pl.BlockSpec(memory_space=pltpu.HBM)
    vmem = pl.BlockSpec(memory_space=pltpu.VMEM)
    groups = sum(2 if level[0] == "d" else 4 for chunk in CHUNKS for level in chunk[0])
    return pl.pallas_call(
        lambda *refs: kernel(max_norm, count, *refs),
        out_shape=(pltpu.VMEM(shape, f32), pltpu.VMEM(shape, f32), pltpu.VMEM(shape, fast.dtype)),
        in_specs=[hbm, hbm, hbm],
        out_specs=(vmem, vmem, vmem),
        scratch_shapes=[
            pltpu.VMEM(shape, f32),
            pltpu.VMEM(shape, fast.dtype),
            pltpu.VMEM(shape, f32),
            pltpu.VMEM(shape, f32),
            pltpu.VMEM(shape, f32),
            pltpu.VMEM(shape, f32),
            pltpu.VMEM((3, 8, 128), f32),
            pltpu.VMEM((22, 8, 128), f32),
            pltpu.VMEM((8, 128), f32),
            pltpu.SemaphoreType.DMA((2 * len(LOADS) + 1,)),
            pltpu.SemaphoreType.DMA((groups,)),
            pltpu.SemaphoreType.DMA((3,)),
            pltpu.SemaphoreType.DMA((2,)),
            pltpu.SemaphoreType.REGULAR((2,)),
        ],
        compiler_params=pltpu.CompilerParams(
            collective_id=0, has_side_effects=True, vmem_limit_bytes=40 * 1024 * 1024
        ),
        name="updated",
    )(*(pltpu.with_memory_space_constraint(x, pltpu.HBM) for x in (slow, fast, momentum)))


def written(*values):
    def run(*refs):
        n = len(values)
        copies = [pltpu.make_async_copy(refs[i], refs[n + i], refs[-1].at[i]) for i in range(n)]
        for copy in copies:
            copy.start()
        for copy in copies:
            copy.wait()

    return pl.pallas_call(
        run,
        out_shape=tuple(pltpu.HBM(x.shape, x.dtype) for x in values),
        in_specs=[pl.BlockSpec(memory_space=pltpu.VMEM)] * len(values),
        out_specs=tuple(pl.BlockSpec(memory_space=pltpu.HBM) for _ in values),
        scratch_shapes=[pltpu.SemaphoreType.DMA((len(values),))],
        compiler_params=pltpu.CompilerParams(vmem_limit_bytes=1024 * 1024),
        name="written",
    )(*(pltpu.with_memory_space_constraint(x, pltpu.VMEM) for x in values))


def body(slow_weights, fast_weights, momentum):
    replicas = lax.axis_size("dp")
    entries = slow_weights.shape[0] * slow_weights.shape[1] * slow_weights.shape[2] * lax.axis_size("mp")
    max_norm = CLIP_LEVEL * math.sqrt(entries)
    values = updated(slow_weights[0], fast_weights[0, 0], momentum[0], max_norm, replicas)
    slow_next, momentum_next, fast_next = written(*values)
    return (slow_next[None], momentum_next[None], fast_next[None, None])


def solution(mesh):
    in_specs = (P(None, None, "mp"), P("dp", None, None, "mp"), P(None, None, "mp"))
    out_specs = (P(None, None, "mp"), P(None, None, "mp"), P("dp", None, None, "mp"))
    return jax.shard_map(body, mesh=mesh, in_specs=in_specs, out_specs=out_specs, check_vma=False)
```
